32 devices in a mesh: gx: 2 (over x), gy: 4 (over z), band: 4 (over y, core).
Axes of the slice: x: 2, y: 2, z: 4, core: 2. Of those that a mesh axis runs over, the one named last changes fastest.
Arguments:
- orbitals: float32 [2, 16, 16, 48, 128], P(None, 'band', 'gx', 'gy'), may hold values from -3 to 3
- external: float32 [16, 48, 128], P('gx', 'gy'), may hold values from 2 to 6
Outputs:
- orbitals_next: float32 [2, 16, 16, 48, 128], P(None, 'band', 'gx', 'gy')
- potential_next: float32 [16, 48, 128], P('gx', 'gy')
The draws below stay inside these ranges and needn't reach their ends.
All inputs are finite; a program needn't handle non-finite values.
Results may differ from the reference program's by a relative error of at most 0.00002.
Values sent between devices are 32-bit elements; how exact they have to be, the bound alone decides.
No kernel may reach another device: no remote copies, remote signals or barrier semaphores. Data moves between devices by JAX's collectives and lax.ppermute only.
A program may use at most 64 MiB of HBM per device.

```python
import jax
import jax.numpy as jnp
from jax import lax

NZ = 128
BANDS = 16
NX = 16
NY = 48


def draw_orbitals(key, part):
    shape = (2, BANDS, NX, NY, NZ)
    first_rows = jnp.arange(NX, dtype=jnp.int32)[:, None, None]
    second_rows = jnp.arange(NY, dtype=jnp.int32)[None, :, None]
    third_rows = jnp.arange(NZ, dtype=jnp.int32)[None, None, :]
    parity = (first_rows + second_rows + third_rows) % 2
    pattern = (1 - 2 * parity).astype(jnp.float32)
    amplitude = jax.random.uniform(key, shape, jnp.float32, 0.5, 2.0)
    return (amplitude * pattern[None, None]).astype(jnp.float32)


def level_of(stream_key, shape, split, low, high):
    def one(axis_at, blocks):
        heights = jax.random.uniform(jax.random.fold_in(jax.random.fold_in(stream_key, 6), axis_at), (blocks,), jnp.float32, low / len(split), high / len(split))
        return jnp.repeat(jnp.exp(heights), shape[axis_at] // blocks).reshape((-1,) + (1,) * (len(shape) - axis_at - 1))

    loudness = one(*split[0])
    for cut in split[1:]:
        loudness = loudness * one(*cut)
    return loudness


def setup_inputs(seed: int = 0) -> dict:
    streams_of = jax.random.split(jax.random.key(seed), 3)
    return {
        "orbitals": draw_orbitals(jax.random.fold_in(streams_of[2], 71), 0),
        "external": jnp.clip(2.0 + 4.0 * jax.random.uniform(streams_of[1], (NX, NY, NZ), jnp.float32) ** level_of(streams_of[1], (NX, NY, NZ), ((0, 2), (1, 4)), -0.2, 0.2), 2.0, 6.0),
    }


step_length = 0.15
exchange_coef = 0.7386
centre_weight = -2.5
near_weight = 4.0 / 3.0
far_weight = -1.0 / 12.0


def shifted(padded, which_axis, offset):
    dimensions = padded.ndim
    selector = []
    for position in range(dimensions):
        if position < dimensions - 3:
            selector.append(slice(None))
        elif position == which_axis:
            selector.append(slice(2 + offset, padded.shape[position] - 2 + offset))
        else:
            selector.append(slice(2, padded.shape[position] - 2))
    return padded[tuple(selector)]


def laplacian(padded):
    dimensions = padded.ndim
    centre = shifted(padded, dimensions - 1, 0)
    summed = 3.0 * centre_weight * centre
    for which_axis in range(dimensions - 3, dimensions):
        summed = summed + near_weight * (shifted(padded, which_axis, 1) + shifted(padded, which_axis, -1))
        summed = summed + far_weight * (shifted(padded, which_axis, 2) + shifted(padded, which_axis, -2))
    return summed


def taylor(values, apply_fn, interval):
    summed = values
    taylor_term = values
    for degree in range(1, 5):
        image = apply_fn(taylor_term)
        factor = interval / degree
        taylor_term = jnp.stack([factor * image[1], -factor * image[0]])
        summed = summed + taylor_term
    return summed


def hamiltonian(values, potential):
    padded = jnp.pad(values, ((0, 0), (2, 2), (2, 2), (2, 2)))
    return -0.5 * laplacian(padded) + potential * values


def reference(orbitals, external):
    density_now = jnp.sum(orbitals * orbitals, axis=(0, 1))
    potential_now = external - exchange_coef * jnp.cbrt(density_now)
    by_band = jnp.moveaxis(orbitals, 1, 0)

    def apply_now(values):
        return hamiltonian(values, potential_now)

    def predict(values):
        return taylor(values, apply_now, step_length)

    predicted = lax.map(predict, by_band)
    density_next = jnp.sum(predicted * predicted, axis=(0, 1))
    potential_next = external - exchange_coef * jnp.cbrt(density_next)

    def apply_next(values):
        return hamiltonian(values, potential_next)

    def finish(values):
        halfway = taylor(values, apply_now, step_length / 2)
        return taylor(halfway, apply_next, step_length / 2)

    result = lax.map(finish, by_band)
    return jnp.moveaxis(result, 0, 1), potential_next
```

```python
import functools

import jax
import jax.numpy as jnp
from jax import lax
from jax.experimental import pallas as pl
from jax.experimental.pallas import tpu as pltpu
from jax.sharding import PartitionSpec as P


step_length = 0.15
exchange_coef = 0.7386
ORDER = 4
WIDE = 2 * ORDER
AXES = ("gx", "gy", "band")
LANES = 128


def corner_depth(dx):
    return 2 * (ORDER - (dx + 1) // 2)


def partner(kind, index, count):
    other = index ^ 1 if kind == 0 else ((index + 1) ^ 1) - 1
    return other if 0 <= other < count else None


class Plan:
    def __init__(self, mesh, shape):
        self.gx, self.gy, self.groups = (mesh.shape[a] for a in AXES)
        self.parts, self.bands, self.rows, self.cols, self.depth = shape
        self.fields = self.parts * self.bands
        self.cells = self.rows * self.cols
        self.xs = tuple(k for k in (0, 1) if k < self.gx - 1)
        self.ys = tuple(k for k in (0, 1) if k < self.gy - 1)
        self.ext_rows = self.rows + 2 * WIDE
        self.ext_cols = self.cols + 2 * WIDE
        self.v_hi = -(-(WIDE + self.cols) // 8) * 8
        self.v_cols = self.v_hi + WIDE
        self.corner = sum(corner_depth(dx) for dx in range(1, WIDE - 1))
        self.v_rows = WIDE // 2
        self.edge_cells = len(self.xs) * (self.corner + self.v_rows) + self.rows

    def pairs(self, kx=None, ky=None, flip=0):
        out = []
        for i in range(self.gx):
            for j in range(self.gy):
                for b in range(self.groups):
                    i2 = i if kx is None else partner(kx, i, self.gx)
                    j2 = j if ky is None else partner(ky, j, self.gy)
                    to = (i, j, b ^ 1) if i2 is None or j2 is None else (i2, j2, b ^ flip)
                    index = lambda t: (t[0] * self.gy + t[1]) * self.groups + t[2]
                    out.append((index((i, j, b)), index(to)))
        return out

    def swap(self, value, **kinds):
        return lax.ppermute(value, AXES, self.pairs(**kinds))

    def above(self, axis, kind):
        return lax.rem(lax.axis_index(axis), 2) == kind

    def far_row(self, hi, dx):
        return jnp.where(hi, WIDE + self.rows + dx - 1, WIDE - dx)

    def source_row(self, hi, dx):
        return jnp.where(hi, dx - 1, self.rows - dx)


def pack_y(plan, fields_ref, out_refs):
    for ky, out in zip(plan.ys, out_refs):
        base = jnp.where(plan.above("gy", ky), plan.cols - WIDE, 0)

        def row(r, carry, out=out, base=base):
            out[pl.ds(r * WIDE, WIDE)] = fields_ref[pl.ds(r * plan.cols + base, WIDE)]
            return carry

        lax.fori_loop(0, plan.rows, row, 0, unroll=True)


def enter_kernel(plan, orb_ref, fields_ref, dens_ref, *rest):
    y_refs, flat = rest[: len(plan.ys)], rest[len(plan.ys)]
    f = plan.fields
    for p in range(plan.parts):
        for b in range(plan.bands):
            for r in range(plan.rows):
                first = r * plan.cols * f + p * plan.bands + b
                flat[pl.ds(first, plan.cols, stride=f), :] = orb_ref[p, b, r]
    for r in range(plan.rows):
        total = None
        for p in range(plan.parts):
            for b in range(plan.bands):
                v = orb_ref[p, b, r]
                total = v * v if total is None else total + v * v
        dens_ref[r] = total
    for c in range(plan.cells):
        fields_ref[c] = flat[c * f : (c + 1) * f, :]
    pack_y(plan, fields_ref, y_refs)


def edge_kernel(plan, *refs):
    nx, ny = len(plan.xs), len(plan.ys)
    refs = list(refs)
    take = lambda n: [refs.pop(0) for _ in range(n)]
    (here,), (ext,) = take(1), take(1)
    more = take(plan.groups // 2 - 1)
    there = [take(plan.groups // 2) for _ in range(nx)]
    ext_x = take(nx)
    far = take(nx)
    (v_here,) = take(1)
    v_there = take(nx)
    out = take(ny)

    def potential(parts, outer):
        total = parts[0][...]
        for q in parts[1:]:
            total = total + q[...]
        return outer[...] - exchange_coef * cube_root(total)

    v_here[...] = potential([here] + more, ext)
    for n in range(nx):
        v_there[n][...] = potential(there[n], ext_x[n])
    for ky, o in zip(plan.ys, out):
        hi = plan.above("gy", ky)
        pick = lambda v: jnp.where(hi, v[plan.cols - WIDE :], v[:WIDE])
        at = 0
        for r in range(plan.rows):
            o[at] = pick(v_here[r])
            at += 1
        for n, kx in enumerate(plan.xs):
            x_hi = plan.above("gx", kx)
            for dx in range(1, plan.v_rows + 1):
                o[at] = pick(v_there[n][plan.source_row(x_hi, dx)])
                at += 1
            for dx in range(1, WIDE - 1):
                size = corner_depth(dx)
                first = plan.source_row(x_hi, dx) * plan.cols + jnp.where(hi, plan.cols - size, 0)
                o[at : at + size] = far[n][pl.ds(first, size)]
                at += size


def cube_root(value):
    root = jnp.exp(jnp.log(value) * (1.0 / 3.0))
    cubed = root * root * root
    better = root * (cubed + 2.0 * value) / (2.0 * cubed + value)
    return jnp.where(root > 1e-10, better, root)


def evolve_kernel(plan, final, *refs):
    nx, ny = len(plan.xs), len(plan.ys)
    refs = list(refs)
    take = lambda n: [refs.pop(0) for _ in range(n)]
    (own,) = take(1)
    far, big, edge = take(nx), take(ny), take(ny)
    (v_here,) = take(1)
    v_there = take(nx)
    if final:
        (orb_ref,) = take(1)
    else:
        (half_ref, dens_ref) = take(2)
        y_refs = take(ny)
    levels = take(ORDER)
    pot = take(1)[0]
    if final:
        flat = take(1)[0]
    rows, cols, f = plan.rows, plan.cols, plan.fields
    wide_cols = plan.ext_cols
    i, j = lax.axis_index("gx"), lax.axis_index("gy")
    h0 = levels[0]

    for r in range(rows):
        h0[pl.ds((WIDE + r) * wide_cols + WIDE, cols)] = own[pl.ds(r * cols, cols)]
        pot[WIDE + r, WIDE : WIDE + cols, :] = 24.0 * v_here[r] + 90.0
    for n, kx in enumerate(plan.xs):
        x_hi = plan.above("gx", kx)
        for dx in range(1, WIDE + 1):
            row, src = plan.far_row(x_hi, dx), plan.source_row(x_hi, dx)
            h0[pl.ds(row * wide_cols + WIDE, cols)] = far[n][pl.ds(src * cols, cols)]
            if dx <= WIDE - 2:
                pot[row, WIDE : WIDE + cols, :] = 24.0 * v_there[n][src] + 90.0
    for n, ky in enumerate(plan.ys):
        hi = plan.above("gy", ky)
        base = jnp.where(hi, WIDE + cols, 0)
        v_base = pl.multiple_of(jnp.where(hi, plan.v_hi, 0), 8)
        at = 0
        for r in range(rows):
            h0[pl.ds((WIDE + r) * wide_cols + base, WIDE)] = big[n][pl.ds(r * WIDE, WIDE)]
            pot[WIDE + r, pl.ds(v_base, WIDE), :] = 24.0 * edge[n][at] + 90.0
            at += 1
        for kx in plan.xs:
            x_hi = plan.above("gx", kx)
            for dx in range(1, plan.v_rows + 1):
                pot[plan.far_row(x_hi, dx), pl.ds(v_base, WIDE), :] = 24.0 * edge[n][at] + 90.0
                at += 1
            for dx in range(1, WIDE - 1):
                size = corner_depth(dx)
                first = plan.far_row(x_hi, dx) * wide_cols + jnp.where(hi, WIDE + cols, WIDE - size)
                h0[pl.ds(first, size)] = edge[n][at : at + size]
                at += size

    def clear_outside(h):
        for at_edge, col in ((j == 0, WIDE - 2), (j == plan.gy - 1, WIDE + cols)):

            @pl.when(at_edge)
            def _(col=col):
                def row(r, carry):
                    h[pl.ds(r * wide_cols + col, 2)] = jnp.zeros((2, f, LANES), jnp.float32)
                    return carry

                lax.fori_loop(0, plan.ext_rows, row, 0)

        for at_edge, row in ((i == 0, WIDE - 2), (i == plan.gx - 1, WIDE + rows)):

            @pl.when(at_edge)
            def _(row=row):
                for r in (row, row + 1):
                    h[pl.ds(r * wide_cols, wide_cols)] = jnp.zeros((wide_cols, f, LANES), jnp.float32)

    lane = lax.broadcasted_iota(jnp.int32, (f, LANES), 1)
    shifts = ((1, lane >= 1), (LANES - 1, lane < LANES - 1), (2, lane >= 2), (LANES - 2, lane < LANES - 2))

    def image(h, row, reach, use):
        base = row * wide_cols
        line = {c: h[base + c] for c in range(WIDE - reach - 2, WIDE - reach + 2)}
        for c in range(WIDE - reach, WIDE + cols + reach):
            line[c + 2] = h[base + c + 2]
            v = line[c]
            z = [jnp.where(keep, pltpu.roll(v, s, 1), 0.0) for s, keep in shifts]
            near = (line[c - 1] + line[c + 1]) + (h[base + c - wide_cols] + h[base + c + wide_cols])
            near = near + (z[0] + z[1])
            outer = (line[c - 2] + line[c + 2]) + (h[base + c - 2 * wide_cols] + h[base + c + 2 * wide_cols])
            outer = outer + (z[2] + z[3])
            cc = c if c < WIDE + cols else c - WIDE - cols + plan.v_hi
            use(base + c, c, (outer - 16.0 * near) + pot[row, cc : cc + 1, :] * v)

    clear_outside(h0)
    for k in range(1, ORDER):
        source, target = levels[k - 1], levels[k]
        reach = 2 * (ORDER - k)

        def store(at, c, value, target=target):
            target[at] = value

        def own_row(r, carry, source=source, reach=reach, store=store):
            image(source, WIDE + r, reach, store)
            return carry

        lax.fori_loop(0, rows, own_row, 0)
        for m in range(1, ORDER - k + 1):
            for kx in plan.xs:
                x_hi = plan.above("gx", kx)

                def far_row(t, carry, m=m, x_hi=x_hi, source=source, reach=reach, store=store):
                    image(source, plan.far_row(x_hi, 2 * m - 1 + t), reach - 2 * m, store)
                    return carry

                lax.fori_loop(0, 2, far_row, 0)
        clear_outside(target)

    sign = jnp.where(lax.broadcasted_iota(jnp.int32, (f, LANES), 0) < plan.bands, 1.0, -1.0)

    def total(s, g):
        a = [(s / 24.0) ** k for k in range(ORDER + 1)]
        even = g[0] - (a[2] / 2) * g[2] + (a[4] / 24) * g[4]
        odd = a[1] * g[1] - (a[3] / 6) * g[3]
        return even + sign * pltpu.roll(odd, plan.bands, 0)

    def last_row(r, carry):
        def finish(at, c, value):
            g = [h[at] for h in levels] + [value]
            half = total(step_length / 2, g)
            cell = r * cols + c - WIDE
            if final:
                flat[pl.ds(pl.multiple_of(cell * f, f), f), :] = half
            else:
                half_ref[cell] = half
                full = total(step_length, g)
                dens_ref[r, c - WIDE : c - WIDE + 1, :] = jnp.sum(full * full, axis=0, keepdims=True)

        image(levels[-1], WIDE + r, 0, finish)
        return carry

    lax.fori_loop(0, rows, last_row, 0)
    if final:
        for p in range(plan.parts):
            for b in range(plan.bands):
                for r in range(rows):
                    first = r * cols * f + p * plan.bands + b
                    orb_ref[p, b, r] = flat[pl.ds(first, cols, stride=f), :]
    else:
        pack_y(plan, half_ref, y_refs)


def call(kernel, outs, scratch=(), flops=1, name=None):
    spec = pl.BlockSpec(memory_space=pltpu.VMEM)
    return lambda *args: pl.pallas_call(
        kernel,
        in_specs=[spec] * len(args),
        out_shape=[jax.ShapeDtypeStruct(s, jnp.float32) for s in outs],
        out_specs=[spec] * len(outs),
        scratch_shapes=list(scratch),
        cost_estimate=pl.CostEstimate(flops=flops, bytes_accessed=1 << 20, transcendentals=0),
        name=name,
    )(*args)


def solution(mesh):
    def body(orbitals, external):
        plan = Plan(mesh, orbitals.shape)
        f, cells, wide = plan.fields, plan.cells, (plan.rows * WIDE, plan.fields, LANES)
        field_shape, plane = (cells, f, LANES), (plan.rows, plan.cols, LANES)
        nx, ny = len(plan.xs), len(plan.ys)
        ext_x = [plan.swap(external, kx=k) for k in plan.xs]

        fields, dens, *big = call(
            functools.partial(enter_kernel, plan),
            [field_shape, plane] + [wide] * ny,
            [pltpu.VMEM((cells * f, LANES), jnp.float32)],
            name="enter",
        )(orbitals)

        def gather(fields, dens, big):
            far = [plan.swap(fields, kx=k) for k in plan.xs]
            dens = dens + plan.swap(dens, flip=1)
            flips = range(2, plan.groups, 2)
            more = [plan.swap(dens, flip=b) for b in flips]
            there = [[plan.swap(dens, kx=k, flip=b) for b in (0, *flips)] for k in plan.xs]
            big = [plan.swap(v, ky=k) for k, v in zip(plan.ys, big)]
            v_here, *rest = call(
                functools.partial(edge_kernel, plan),
                [plane] * (1 + nx) + [(plan.edge_cells, f, LANES)] * ny,
                name="edge",
            )(dens, external, *more, *sum(there, []), *ext_x, *far)
            v_there, edge = rest[:nx], rest[nx:]
            edge = [plan.swap(v, ky=k) for k, v in zip(plan.ys, edge)]
            return [*far, *big, *edge, v_here, *v_there], v_here

        scratch = [pltpu.VMEM((plan.ext_rows * plan.ext_cols, f, LANES), jnp.float32)] * ORDER
        scratch.append(pltpu.VMEM((plan.ext_rows, plan.v_cols, LANES), jnp.float32))
        arrived, _ = gather(fields, dens, big)
        half, dens, *big = call(
            functools.partial(evolve_kernel, plan, False),
            [field_shape, plane] + [wide] * ny,
            scratch,
            name="first",
        )(fields, *arrived)
        arrived, potential = gather(half, dens, big)
        (result,) = call(
            functools.partial(evolve_kernel, plan, True),
            [orbitals.shape],
            scratch + [pltpu.VMEM((cells * f, LANES), jnp.float32)],
            name="second",
        )(half, *arrived)
        return result, potential

    in_specs = (P(None, "band", "gx", "gy", None), P("gx", "gy", None))
    out_specs = (P(None, "band", "gx", "gy", None), P("gx", "gy", None))
    return jax.shard_map(body, mesh=mesh, in_specs=in_specs, out_specs=out_specs, check_vma=False)
```

```python
import functools

import jax
import jax.numpy as jnp
from jax import lax
from jax.experimental import pallas as pl
from jax.experimental.pallas import tpu as pltpu
from jax.sharding import PartitionSpec as P


step_length = 0.15
exchange_coef = 0.7386
ORDER = 4
WIDE = 2 * ORDER
AXES = ("gx", "gy", "band")
LANES = 128


def corner_depth(d):
    return 2 * (ORDER - (d + 1) // 2)


def partner(kind, index, count):
    other = index ^ 1 if kind == 0 else ((index + 1) ^ 1) - 1
    return other if 0 <= other < count else None


class Plan:
    def __init__(self, mesh, shape):
        self.gx, self.gy, self.groups = (mesh.shape[a] for a in AXES)
        self.parts, self.bands, self.cols, self.rows, self.depth = shape
        self.fields = self.parts * self.bands
        self.cells = self.rows * self.cols
        self.xs = tuple(k for k in (0, 1) if k < self.gx - 1)
        self.ys = tuple(k for k in (0, 1) if k < self.gy - 1)
        self.ext_rows = self.rows + 2 * WIDE
        self.ext_cols = self.cols + 2 * WIDE
        self.corner = sum(corner_depth(d) for d in range(1, WIDE - 1))
        self.v_cols = WIDE // 2
        self.edge_cells = len(self.xs) * (self.corner + self.v_cols) + WIDE
        self.wide_cells = WIDE * self.rows

    def pairs(self, kx=None, ky=None, flip=0):
        index = lambda i, j, b: (i * self.gy + j) * self.groups + b
        out = []
        for i in range(self.gx):
            for j in range(self.gy):
                for b in range(self.groups):
                    i2 = i if kx is None else partner(kx, i, self.gx)
                    j2 = j if ky is None else partner(ky, j, self.gy)
                    to = (i, j, b ^ 1) if i2 is None or j2 is None else (i2, j2, b ^ flip)
                    out.append((index(i, j, b), index(*to)))
        return out

    def swap(self, value, **kinds):
        return lax.ppermute(value, AXES, self.pairs(**kinds))

    def above(self, axis, kind):
        return lax.rem(lax.axis_index(axis), 2) == kind

    def near(self, hi, size, extent):
        return 0 if size == extent else jnp.where(hi, extent - size, 0)

    def beyond(self, hi, size, extent):
        return jnp.where(hi, WIDE + extent, WIDE - size)

    def at_partner(self, hi, size, extent):
        return 0 if size == extent else jnp.where(hi, 0, extent - size)

    def span(self, reach):
        if len(self.xs) == 2:
            return WIDE - reach, self.rows + 2 * reach
        if not self.xs:
            return WIDE, self.rows
        return jnp.where(self.above("gx", 0), WIDE, WIDE - reach), self.rows + reach


def pack_y(plan, fields_ref, out_refs):
    for ky, out in zip(plan.ys, out_refs):
        base = plan.near(plan.above("gy", ky), WIDE, plan.cols)
        for c in range(WIDE):
            out[pl.ds(c * plan.rows, plan.rows)] = fields_ref[pl.ds((base + c) * plan.rows, plan.rows)]


def enter_kernel(plan, orb_ref, fields_ref, dens_ref, *rest):
    y_refs, flat = rest[: len(plan.ys)], rest[len(plan.ys)]
    f, rows = plan.fields, plan.rows
    for c in range(plan.cols):
        total = None
        for p in range(plan.parts):
            for b in range(plan.bands):
                v = orb_ref[p, b, c]
                flat[pl.ds(c * rows * f + p * plan.bands + b, rows, stride=f), :] = v
                total = v * v if total is None else total + v * v
        dens_ref[c] = total
        for r in range(c * rows, (c + 1) * rows):
            fields_ref[r] = flat[r * f : (r + 1) * f, :]
    pack_y(plan, fields_ref, y_refs)


def cube_root(value):
    root = jnp.exp(jnp.log(value) * (1.0 / 3.0))
    cubed = root * root * root
    better = root * (cubed + 2.0 * value) / (2.0 * cubed + value)
    return jnp.where(root > 1e-10, better, root)


def edge_kernel(plan, *refs):
    nx, ny = len(plan.xs), len(plan.ys)
    refs = list(refs)
    take = lambda n: [refs.pop(0) for _ in range(n)]
    (here,), (ext,) = take(1), take(1)
    more = take(plan.groups // 2 - 1)
    there = [take(plan.groups // 2) for _ in range(nx)]
    ext_x = take(nx)
    far = take(nx)
    (v_here,) = take(1)
    v_there = take(nx)
    out = take(ny)

    def potential(parts, outer):
        total = parts[0][...]
        for q in parts[1:]:
            total = total + q[...]
        return outer[...] - exchange_coef * cube_root(total)

    v_here[...] = potential([here] + more, ext)
    for n in range(nx):
        v_there[n][...] = potential(there[n], ext_x[n])
    for ky, o in zip(plan.ys, out):
        hi = plan.above("gy", ky)
        o[0:WIDE] = v_here[pl.ds(plan.near(hi, WIDE, plan.cols), WIDE)]
        at = WIDE
        for n, kx in enumerate(plan.xs):
            x_hi = plan.above("gx", kx)
            o[at : at + plan.v_cols] = v_there[n][pl.ds(plan.near(hi, plan.v_cols, plan.cols), plan.v_cols)]
            at += plan.v_cols
            for d in range(1, WIDE - 1):
                size = corner_depth(d)
                col = jnp.where(hi, plan.cols - d, d - 1)
                first = col * plan.rows + plan.at_partner(x_hi, size, plan.rows)
                o[at : at + size] = far[n][pl.ds(first, size)]
                at += size


def evolve_kernel(plan, final, *refs):
    nx, ny = len(plan.xs), len(plan.ys)
    refs = list(refs)
    take = lambda n: [refs.pop(0) for _ in range(n)]
    (own,) = take(1)
    far, big, edge = take(nx), take(ny), take(ny)
    (v_here,) = take(1)
    v_there = take(nx)
    if final:
        (orb_ref,) = take(1)
    else:
        (half_ref, dens_ref) = take(2)
        y_refs = take(ny)
    levels = take(ORDER)
    (pot,) = take(1)
    if final:
        (flat,) = take(1)
    rows, cols, f = plan.rows, plan.cols, plan.fields
    long = plan.ext_rows
    i, j = lax.axis_index("gx"), lax.axis_index("gy")
    h0 = levels[0]

    def put_potential(first, v, count):
        scaled = 24.0 * v + 90.0
        for t in range(count):
            pot[first + t] = jnp.broadcast_to(scaled[t : t + 1, :], (f, LANES))

    for c in range(cols):
        at = (WIDE + c) * long + WIDE
        h0[at : at + rows] = own[c * rows : (c + 1) * rows]
        put_potential(at, v_here[c], rows)
    for n, kx in enumerate(plan.xs):
        x_hi = plan.above("gx", kx)
        row, src = plan.beyond(x_hi, WIDE, rows), plan.at_partner(x_hi, WIDE, rows)
        for c in range(cols):
            at = (WIDE + c) * long + row
            h0[pl.ds(at, WIDE)] = far[n][pl.ds(c * rows + src, WIDE)]
            put_potential(at, v_there[n][c, pl.ds(src, WIDE), :], WIDE)
    for n, ky in enumerate(plan.ys):
        hi = plan.above("gy", ky)
        base = plan.beyond(hi, WIDE, cols)
        for c in range(WIDE):
            at = (base + c) * long + WIDE
            h0[pl.ds(at, rows)] = big[n][pl.ds(c * rows, rows)]
            put_potential(at, edge[n][c], rows)
        at = WIDE
        for kx in plan.xs:
            x_hi = plan.above("gx", kx)
            row, src = plan.beyond(x_hi, WIDE, rows), plan.at_partner(x_hi, WIDE, rows)
            first = plan.beyond(hi, plan.v_cols, cols)
            for c in range(plan.v_cols):
                put_potential((first + c) * long + row, edge[n][at, pl.ds(src, WIDE), :], WIDE)
                at += 1
            for d in range(1, WIDE - 1):
                size = corner_depth(d)
                col = jnp.where(hi, WIDE + cols + d - 1, WIDE - d)
                h0[pl.ds(col * long + plan.beyond(x_hi, size, rows), size)] = edge[n][at : at + size]
                at += size

    def clear_outside(h):
        for outside, col in ((j == 0, WIDE - 2), (j == plan.gy - 1, WIDE + cols)):

            @pl.when(outside)
            def _(col=col):
                for c in (col, col + 1):
                    h[c * long : (c + 1) * long] = jnp.zeros((long, f, LANES), jnp.float32)

        for outside, row in ((i == 0, WIDE - 2), (i == plan.gx - 1, WIDE + rows)):

            @pl.when(outside)
            def _(row=row):
                for c in range(plan.ext_cols):
                    h[c * long + row : c * long + row + 2] = jnp.zeros((2, f, LANES), jnp.float32)

    lane = lax.broadcasted_iota(jnp.int32, (f, LANES), 1)
    shifts = ((1, lane >= 1), (LANES - 1, lane < LANES - 1), (2, lane >= 2), (LANES - 2, lane < LANES - 2))

    def image(h, first, count, use):
        line = [h[first + t] for t in range(-2, 2)]
        for t in range(count):
            at = first + t
            line.append(h[at + 2])
            v = line[2]
            z = [jnp.where(keep, pltpu.roll(v, s, 1), 0.0) for s, keep in shifts]
            near = (line[1] + line[3]) + (h[at - long] + h[at + long]) + (z[0] + z[1])
            outer = (line[0] + line[4]) + (h[at - 2 * long] + h[at + 2 * long]) + (z[2] + z[3])
            use(at, t, (outer - 16.0 * near) + pot[at] * v)
            line.pop(0)

    clear_outside(h0)
    for k in range(1, ORDER):
        source, target = levels[k - 1], levels[k]

        def column(col, reach, source=source, target=target):
            row, count = plan.span(reach)

            def store(at, t, value):
                target[at] = value

            image(source, col * long + row, count, store)

        reach = 2 * (ORDER - k)

        @pl.loop(0, cols)
        def _(c, reach=reach, column=column):
            column(WIDE + c, reach)

        for m in range(1, ORDER - k + 1):
            if plan.ys:

                @pl.loop(0, 4)
                def _(t, m=m, reach=reach, column=column):
                    col = jnp.where(t < 2, WIDE - 2 * m, WIDE + cols + 2 * m - 4)
                    column(col + t, reach - 2 * m)

        clear_outside(target)

    sign = jnp.where(lax.broadcasted_iota(jnp.int32, (f, LANES), 0) < plan.bands, 1.0, -1.0)

    def total(s, g):
        a = [(s / 24.0) ** k for k in range(ORDER + 1)]
        even = g[0] - (a[2] / 2) * g[2] + (a[4] / 24) * g[4]
        odd = a[1] * g[1] - (a[3] / 6) * g[3]
        return even + sign * pltpu.roll(odd, plan.bands, 0)

    @pl.loop(0, cols)
    def _(c):
        def finish(at, t, value):
            g = [h[at] for h in levels] + [value]
            half = total(step_length / 2, g)
            cell = c * rows + t
            if final:
                flat[pl.ds(pl.multiple_of(cell * f, f), f), :] = half
            else:
                half_ref[cell] = half
                full = total(step_length, g)
                dens_ref[c, t : t + 1, :] = jnp.sum(full * full, axis=0, keepdims=True)

        image(levels[-1], (WIDE + c) * long + WIDE, rows, finish)

    if final:
        for c in range(cols):
            for p in range(plan.parts):
                for b in range(plan.bands):
                    first = c * rows * f + p * plan.bands + b
                    orb_ref[p, b, c] = flat[pl.ds(first, rows, stride=f), :]
    else:
        pack_y(plan, half_ref, y_refs)


def call(kernel, outs, scratch=(), limit=8, name=None):
    spec = pl.BlockSpec(memory_space=pltpu.VMEM)
    return lambda *args: pl.pallas_call(
        kernel,
        out_shape=[jax.ShapeDtypeStruct(s, jnp.float32) for s in outs],
        in_specs=[spec] * len(args),
        out_specs=[spec] * len(outs),
        scratch_shapes=list(scratch),
        compiler_params=pltpu.CompilerParams(vmem_limit_bytes=limit << 20),
        name=name,
    )(*args)


def solution(mesh):
    def body(orbitals, external):
        orbitals, external = jnp.swapaxes(orbitals, 2, 3), jnp.swapaxes(external, 0, 1)
        plan = Plan(mesh, orbitals.shape)
        f, cells = plan.fields, plan.cells
        field_shape, plane = (cells, f, LANES), (plan.cols, plan.rows, LANES)
        wide = (plan.wide_cells, f, LANES)
        nx, ny = len(plan.xs), len(plan.ys)
        ext_x = [plan.swap(external, kx=k) for k in plan.xs]

        fields, dens, *big = call(
            functools.partial(enter_kernel, plan),
            [field_shape, plane] + [wide] * ny,
            [pltpu.VMEM((cells * f, LANES), jnp.float32)],
            name="enter",
        )(orbitals)

        def gather(fields, dens, big):
            far = [plan.swap(fields, kx=k) for k in plan.xs]
            dens = dens + plan.swap(dens, flip=1)
            flips = range(2, plan.groups, 2)
            more = [plan.swap(dens, flip=b) for b in flips]
            there = [[plan.swap(dens, kx=k, flip=b) for b in (0, *flips)] for k in plan.xs]
            big = [plan.swap(v, ky=k) for k, v in zip(plan.ys, big)]
            v_here, *rest = call(
                functools.partial(edge_kernel, plan),
                [plane] * (1 + nx) + [(plan.edge_cells, f, LANES)] * ny,
                name="edge",
            )(dens, external, *more, *sum(there, []), *ext_x, *far)
            v_there, edge = rest[:nx], rest[nx:]
            edge = [plan.swap(v, ky=k) for k, v in zip(plan.ys, edge)]
            return [*far, *big, *edge, v_here, *v_there], v_here

        extended = pltpu.VMEM((plan.ext_rows * plan.ext_cols, f, LANES), jnp.float32)
        scratch = [extended] * (ORDER + 1)
        arrived, _ = gather(fields, dens, big)
        half, dens, *big = call(
            functools.partial(evolve_kernel, plan, False),
            [field_shape, plane] + [wide] * ny,
            scratch,
            limit=24,
            name="first",
        )(fields, *arrived)
        arrived, potential = gather(half, dens, big)
        (result,) = call(
            functools.partial(evolve_kernel, plan, True),
            [orbitals.shape],
            scratch + [pltpu.VMEM((cells * f, LANES), jnp.float32)],
            limit=24,
            name="second",
        )(half, *arrived)
        return jnp.swapaxes(result, 2, 3), jnp.swapaxes(potential, 0, 1)

    in_specs = (P(None, "band", "gx", "gy", None), P("gx", "gy", None))
    out_specs = (P(None, "band", "gx", "gy", None), P("gx", "gy", None))
    return jax.shard_map(body, mesh=mesh, in_specs=in_specs, out_specs=out_specs, check_vma=False)
```

```python
import functools

import jax
import jax.numpy as jnp
from jax import lax
from jax.experimental import pallas as pl
from jax.experimental.pallas import tpu as pltpu
from jax.sharding import PartitionSpec as P


step_length = 0.15
exchange_coef = 0.7386
ORDER = 4
WIDE = 2 * ORDER
AXES = ("gx", "gy", "band")
LANES = 128


def corner_depth(d):
    return 2 * (ORDER - (d + 1) // 2)


def partner(kind, index, count):
    other = index ^ 1 if kind == 0 else ((index + 1) ^ 1) - 1
    return other if 0 <= other < count else None


def divisor(count, limit):
    return max(n for n in range(1, limit + 1) if count % n == 0)


class Plan:
    def __init__(self, mesh, shape):
        self.gx, self.gy, self.groups = (mesh.shape[a] for a in AXES)
        self.parts, self.bands, self.cols, self.rows, self.depth = shape
        self.fields = self.parts * self.bands
        self.cells = self.rows * self.cols
        self.xs = tuple(k for k in (0, 1) if k < self.gx - 1)
        self.ys = tuple(k for k in (0, 1) if k < self.gy - 1)
        self.ext_rows = self.rows + 2 * WIDE
        self.ext_cols = self.cols + 2 * WIDE
        self.corner = sum(corner_depth(d) for d in range(1, WIDE - 1))
        self.v_cols = WIDE // 2
        self.edge_cells = len(self.xs) * self.v_cols + WIDE
        self.wide_cells = WIDE * self.rows

    def pairs(self, kx=None, ky=None, flip=0):
        index = lambda i, j, b: (i * self.gy + j) * self.groups + b
        out = []
        for i in range(self.gx):
            for j in range(self.gy):
                for b in range(self.groups):
                    i2 = i if kx is None else partner(kx, i, self.gx)
                    j2 = j if ky is None else partner(ky, j, self.gy)
                    to = (i, j, b ^ 1) if i2 is None or j2 is None else (i2, j2, b ^ flip)
                    out.append((index(i, j, b), index(*to)))
        return out

    def swap(self, value, **kinds):
        return lax.ppermute(value, AXES, self.pairs(**kinds))

    def above(self, axis, kind):
        return lax.rem(lax.axis_index(axis), 2) == kind

    def near(self, hi, size, extent):
        return 0 if size == extent else jnp.where(hi, extent - size, 0)

    def beyond(self, hi, size, extent):
        return jnp.where(hi, WIDE + extent, WIDE - size)

    def at_partner(self, hi, size, extent):
        return 0 if size == extent else jnp.where(hi, 0, extent - size)

    def span(self, reach):
        if len(self.xs) == 2:
            return WIDE - reach, self.rows + 2 * reach
        if not self.xs:
            return WIDE, self.rows
        return jnp.where(self.above("gx", 0), WIDE, WIDE - reach), self.rows + reach


def pack(plan, fields_ref, out_refs):
    out_refs = list(out_refs)
    for ky in plan.ys:
        base, out = plan.near(plan.above("gy", ky), WIDE, plan.cols), out_refs.pop(0)
        for c in range(WIDE):
            out[pl.ds(c * plan.rows, plan.rows)] = fields_ref[pl.ds((base + c) * plan.rows, plan.rows)]
    for ky in plan.ys:
        hi = plan.above("gy", ky)
        for kx in plan.xs:
            x_hi, out, at = plan.above("gx", kx), out_refs.pop(0), 0
            for d in range(1, WIDE - 1):
                size = corner_depth(d)
                col = jnp.where(hi, plan.cols - d, d - 1)
                out[at : at + size] = fields_ref[pl.ds(col * plan.rows + plan.near(x_hi, size, plan.rows), size)]
                at += size


def enter_kernel(plan, orb_ref, fields_ref, dens_ref, *rest):
    *packed, flat = rest
    f, rows = plan.fields, plan.rows
    for c in range(plan.cols):
        total = None
        for p in range(plan.parts):
            for b in range(plan.bands):
                v = orb_ref[p, b, c]
                flat[pl.ds(c * rows * f + p * plan.bands + b, rows, stride=f), :] = v
                total = v * v if total is None else total + v * v
        dens_ref[c] = total
        for r in range(c * rows, (c + 1) * rows):
            fields_ref[r] = flat[r * f : (r + 1) * f, :]
    pack(plan, fields_ref, packed)


def cube_root(value):
    root = jnp.exp(jnp.log(value) * (1.0 / 3.0))
    cubed = root * root * root
    better = root * (cubed + 2.0 * value) / (2.0 * cubed + value)
    return jnp.where(root > 1e-10, better, root)


def potential_kernel(ext_ref, *refs):
    *parts, out = refs
    total = parts[0][...]
    for q in parts[1:]:
        total = total + q[...]
    out[...] = ext_ref[...] - exchange_coef * cube_root(total)


def edge_kernel(plan, v_here, *refs):
    nx = len(plan.xs)
    v_there, out = refs[:nx], refs[nx:]
    for ky, o in zip(plan.ys, out):
        hi = plan.above("gy", ky)
        o[0:WIDE] = v_here[pl.ds(plan.near(hi, WIDE, plan.cols), WIDE)]
        for n in range(nx):
            at = WIDE + n * plan.v_cols
            o[at : at + plan.v_cols] = v_there[n][pl.ds(plan.near(hi, plan.v_cols, plan.cols), plan.v_cols)]


def evolve_kernel(plan, final, *refs):
    nx, ny = len(plan.xs), len(plan.ys)
    refs = list(refs)
    take = lambda n: [refs.pop(0) for _ in range(n)]
    (own,) = take(1)
    far, big = take(nx), take(ny)
    corners = [take(nx) for _ in range(ny)]
    (v_here,) = take(1)
    v_there, edge = take(nx), take(ny)
    if final:
        orb_ref, v_out = take(2)
    else:
        (half_ref, dens_ref) = take(2)
        packed = take(ny + nx * ny)
    levels = take(ORDER)
    (pot,) = take(1)
    if final:
        (flat,) = take(1)
    rows, cols, f = plan.rows, plan.cols, plan.fields
    long = plan.ext_rows
    i, j = lax.axis_index("gx"), lax.axis_index("gy")
    h0 = levels[0]

    def put_potential(first, v, count):
        scaled = 24.0 * v + 90.0
        for t in range(count):
            pot[first + t] = jnp.broadcast_to(scaled[t : t + 1, :], (f, LANES))

    for c in range(cols):
        at = (WIDE + c) * long + WIDE
        h0[at : at + rows] = own[c * rows : (c + 1) * rows]
        put_potential(at, v_here[c], rows)
    for n, kx in enumerate(plan.xs):
        x_hi = plan.above("gx", kx)
        row, src = plan.beyond(x_hi, WIDE, rows), plan.at_partner(x_hi, WIDE, rows)
        for c in range(cols):
            at = (WIDE + c) * long + row
            h0[pl.ds(at, WIDE)] = far[n][pl.ds(c * rows + src, WIDE)]
            put_potential(at, v_there[n][c, pl.ds(src, WIDE), :], WIDE)
    for n, ky in enumerate(plan.ys):
        hi = plan.above("gy", ky)
        base = plan.beyond(hi, WIDE, cols)
        for c in range(WIDE):
            at = (base + c) * long + WIDE
            h0[pl.ds(at, rows)] = big[n][pl.ds(c * rows, rows)]
            put_potential(at, edge[n][c], rows)
        for n_x, kx in enumerate(plan.xs):
            at = WIDE + n_x * plan.v_cols
            x_hi = plan.above("gx", kx)
            row, src = plan.beyond(x_hi, WIDE, rows), plan.at_partner(x_hi, WIDE, rows)
            first = plan.beyond(hi, plan.v_cols, cols)
            for c in range(plan.v_cols):
                put_potential((first + c) * long + row, edge[n][at + c, pl.ds(src, WIDE), :], WIDE)
            at = 0
            for d in range(1, WIDE - 1):
                size = corner_depth(d)
                col = jnp.where(hi, WIDE + cols + d - 1, WIDE - d)
                h0[pl.ds(col * long + plan.beyond(x_hi, size, rows), size)] = corners[n][n_x][at : at + size]
                at += size

    def clear_outside(h):
        for outside, col in ((j == 0, WIDE - 2), (j == plan.gy - 1, WIDE + cols)):

            @pl.when(outside)
            def _(col=col):
                for c in (col, col + 1):
                    h[c * long : (c + 1) * long] = jnp.zeros((long, f, LANES), jnp.float32)

        for outside, row in ((i == 0, WIDE - 2), (i == plan.gx - 1, WIDE + rows)):

            @pl.when(outside)
            def _(row=row):
                for c in range(plan.ext_cols):
                    h[c * long + row : c * long + row + 2] = jnp.zeros((2, f, LANES), jnp.float32)

    lane = lax.broadcasted_iota(jnp.int32, (f, LANES), 1)
    shifts = ((1, lane >= 1), (LANES - 1, lane < LANES - 1), (2, lane >= 2), (LANES - 2, lane < LANES - 2))

    def image(h, first, count, use):
        line = [h[first + t] for t in range(-2, 2)]
        for t in range(count):
            at = first + t
            line.append(h[at + 2])
            v = line[2]
            z = [jnp.where(keep, pltpu.roll(v, s, 1), 0.0) for s, keep in shifts]
            near = (line[1] + line[3]) + (h[at - long] + h[at + long]) + (z[0] + z[1])
            outer = (line[0] + line[4]) + (h[at - 2 * long] + h[at + 2 * long]) + (z[2] + z[3])
            use(at, t, (outer - 16.0 * near) + pot[at] * v)
            line.pop(0)

    clear_outside(h0)
    for k in range(1, ORDER):
        source, target = levels[k - 1], levels[k]

        def column(col, reach, source=source, target=target):
            row, count = plan.span(reach)

            def store(at, t, value):
                target[at] = value

            image(source, col * long + row, count, store)

        reach = 2 * (ORDER - k)

        @pl.loop(0, cols, unroll=divisor(cols, 6))
        def _(c, reach=reach, column=column):
            column(WIDE + c, reach)

        for m in range(1, ORDER - k + 1):
            if plan.ys:

                @pl.loop(0, 4, unroll=4)
                def _(t, m=m, reach=reach, column=column):
                    col = jnp.where(t < 2, WIDE - 2 * m, WIDE + cols + 2 * m - 4)
                    column(col + t, reach - 2 * m)

        clear_outside(target)

    sign = jnp.where(lax.broadcasted_iota(jnp.int32, (f, LANES), 0) < plan.bands, 1.0, -1.0)

    def total(s, g):
        a = [(s / 24.0) ** k for k in range(ORDER + 1)]
        even = g[0] - (a[2] / 2) * g[2] + (a[4] / 24) * g[4]
        odd = a[1] * g[1] - (a[3] / 6) * g[3]
        return even + sign * pltpu.roll(odd, plan.bands, 0)

    @pl.loop(0, cols, unroll=divisor(cols, 6))
    def _(c):
        def finish(at, t, value):
            g = [h[at] for h in levels] + [value]
            half = total(step_length / 2, g)
            cell = c * rows + t
            if final:
                flat[pl.ds(pl.multiple_of(cell * f, f), f), :] = half
            else:
                half_ref[cell] = half
                full = total(step_length, g)
                dens_ref[c, t : t + 1, :] = jnp.sum(full * full, axis=0, keepdims=True)

        image(levels[-1], (WIDE + c) * long + WIDE, rows, finish)

    if final:
        v_out[...] = v_here[...]
        for c in range(cols):
            for p in range(plan.parts):
                for b in range(plan.bands):
                    first = c * rows * f + p * plan.bands + b
                    orb_ref[p, b, c] = flat[pl.ds(first, rows, stride=f), :]
    else:
        pack(plan, half_ref, packed)


def call(kernel, outs, scratch=(), limit=8):
    spec = pl.BlockSpec(memory_space=pltpu.VMEM)
    return lambda *args: pl.pallas_call(
        kernel,
        out_shape=[jax.ShapeDtypeStruct(s, jnp.float32) for s in outs],
        in_specs=[spec] * len(args),
        out_specs=[spec] * len(outs),
        scratch_shapes=list(scratch),
        compiler_params=pltpu.CompilerParams(vmem_limit_bytes=limit << 20),
    )(*args)


def solution(mesh):
    def body(orbitals, external):
        orbitals, external = jnp.swapaxes(orbitals, 2, 3), jnp.swapaxes(external, 0, 1)
        plan = Plan(mesh, orbitals.shape)
        f, cells = plan.fields, plan.cells
        field_shape, plane = (cells, f, LANES), (plan.cols, plan.rows, LANES)
        wide = (plan.wide_cells, f, LANES)
        nx, ny = len(plan.xs), len(plan.ys)
        packed = [wide] * ny + [(plan.corner, f, LANES)] * (nx * ny)

        fields, dens, *out = call(
            functools.partial(enter_kernel, plan),
            [field_shape, plane] + packed,
            [pltpu.VMEM((cells * f, LANES), jnp.float32)],
        )(orbitals)

        def gather(fields, dens, out):
            def swap(value, **kinds):
                return plan.swap(value, **kinds)

            far = [swap(fields, kx=k) for k in plan.xs]
            big = [swap(v, ky=k) for k, v in zip(plan.ys, out)]
            both = [(ky, kx) for ky in plan.ys for kx in plan.xs]
            corners = [swap(v, kx=kx, ky=ky) for (ky, kx), v in zip(both, out[ny:])]
            dens = dens + swap(dens, flip=1)
            more = [swap(dens, flip=b) for b in range(2, plan.groups, 2)]
            (v_here,) = call(potential_kernel, [plane])(external, dens, *more)
            v_there = [swap(v_here, kx=k) for k in plan.xs]
            edge = call(
                functools.partial(edge_kernel, plan), [(plan.edge_cells, plan.rows, LANES)] * ny
            )(v_here, *v_there)
            edge = [swap(v, ky=k) for k, v in zip(plan.ys, edge)]
            return [*far, *big, *corners, v_here, *v_there, *edge]

        extended = pltpu.VMEM((plan.ext_rows * plan.ext_cols, f, LANES), jnp.float32)
        scratch = [extended] * (ORDER + 1)
        arrived = gather(fields, dens, out)
        half, dens, *out = call(
            functools.partial(evolve_kernel, plan, False), [field_shape, plane] + packed, scratch, limit=24
        )(fields, *arrived)
        arrived = gather(half, dens, out)
        result, potential = call(
            functools.partial(evolve_kernel, plan, True),
            [orbitals.shape, plane],
            scratch + [pltpu.VMEM((cells * f, LANES), jnp.float32)],
            limit=24,
        )(half, *arrived)
        return jnp.swapaxes(result, 2, 3), jnp.swapaxes(potential, 0, 1)

    in_specs = (P(None, "band", "gx", "gy", None), P("gx", "gy", None))
    out_specs = (P(None, "band", "gx", "gy", None), P("gx", "gy", None))
    return jax.shard_map(body, mesh=mesh, in_specs=in_specs, out_specs=out_specs, check_vma=False)
```

```python
import functools

import jax
import jax.numpy as jnp
from jax import lax
from jax.experimental import pallas as pl
from jax.experimental.pallas import tpu as pltpu
from jax.sharding import PartitionSpec as P


step_length = 0.15
exchange_coef = 0.7386
ORDER = 4
WIDE = 2 * ORDER
AXES = ("gx", "gy", "band")
LANES = 128


def corner_depth(d):
    return 2 * (ORDER - (d + 1) // 2)


def partner(kind, index, count):
    other = index ^ 1 if kind == 0 else ((index + 1) ^ 1) - 1
    return other if 0 <= other < count else None


def divisor(count, limit):
    return max(n for n in range(1, limit + 1) if count % n == 0)


class Plan:
    def __init__(self, mesh, shape):
        self.gx, self.gy, self.groups = (mesh.shape[a] for a in AXES)
        self.parts, self.bands, self.cols, self.rows, self.depth = shape
        self.fields = self.parts * self.bands
        self.cells = self.rows * self.cols
        self.xs = tuple(k for k in (0, 1) if k < self.gx - 1)
        self.ys = tuple(k for k in (0, 1) if k < self.gy - 1)
        self.ext_rows = self.rows + 2 * WIDE
        self.ext_cols = self.cols + 2 * WIDE
        self.corner = sum(corner_depth(d) for d in range(1, WIDE - 1))
        self.v_cols = WIDE // 2
        self.edge_cells = len(self.xs) * (self.corner + self.v_cols) + WIDE
        depth = [min(c + 1, self.cols - c) for c in range(self.cols)]
        self.soon = [corner_depth(d) if d < WIDE - 1 else 0 for d in depth]
        self.soon_at = [sum(self.soon[:c]) for c in range(self.cols + 1)]
        self.late_at = [c * WIDE - self.soon_at[c] for c in range(self.cols + 1)]
        self.wide_cells = WIDE * self.rows

    def pairs(self, kx=None, ky=None, flip=0):
        index = lambda i, j, b: (i * self.gy + j) * self.groups + b
        out = []
        for i in range(self.gx):
            for j in range(self.gy):
                for b in range(self.groups):
                    i2 = i if kx is None else partner(kx, i, self.gx)
                    j2 = j if ky is None else partner(ky, j, self.gy)
                    to = (i, j, b ^ 1) if i2 is None or j2 is None else (i2, j2, b ^ flip)
                    out.append((index(i, j, b), index(*to)))
        return out

    def swap(self, value, **kinds):
        return lax.ppermute(value, AXES, self.pairs(**kinds))

    def above(self, axis, kind):
        return lax.rem(lax.axis_index(axis), 2) == kind

    def near(self, hi, size, extent):
        return 0 if size == extent else jnp.where(hi, extent - size, 0)

    def beyond(self, hi, size, extent):
        return jnp.where(hi, WIDE + extent, WIDE - size)

    def at_partner(self, hi, size, extent):
        return 0 if size == extent else jnp.where(hi, 0, extent - size)

    def span(self, reach):
        if len(self.xs) == 2:
            return WIDE - reach, self.rows + 2 * reach
        if not self.xs:
            return WIDE, self.rows
        return jnp.where(self.above("gx", 0), WIDE, WIDE - reach), self.rows + reach


def pack(plan, fields_ref, out_refs):
    nx, ny = len(plan.xs), len(plan.ys)
    rows = plan.rows
    for ky, out in zip(plan.ys, out_refs[:ny]):
        base = plan.near(plan.above("gy", ky), WIDE, plan.cols)
        for c in range(WIDE):
            out[pl.ds(c * rows, rows)] = fields_ref[pl.ds((base + c) * rows, rows)]
    for kx, soon, late in zip(plan.xs, out_refs[ny : ny + nx], out_refs[ny + nx :]):
        hi = plan.above("gx", kx)
        for c, n in enumerate(plan.soon):
            if n:
                soon[plan.soon_at[c] : plan.soon_at[c + 1]] = fields_ref[pl.ds(c * rows + plan.near(hi, n, rows), n)]
            first = c * rows + jnp.where(hi, rows - WIDE, n)
            late[plan.late_at[c] : plan.late_at[c + 1]] = fields_ref[pl.ds(first, WIDE - n)]


def enter_kernel(plan, orb_ref, fields_ref, dens_ref, *rest):
    *packed, flat = rest
    f, rows = plan.fields, plan.rows
    for c in range(plan.cols):
        total = None
        for p in range(plan.parts):
            for b in range(plan.bands):
                v = orb_ref[p, b, c]
                flat[pl.ds(c * rows * f + p * plan.bands + b, rows, stride=f), :] = v
                total = v * v if total is None else total + v * v
        dens_ref[c] = total
        for r in range(c * rows, (c + 1) * rows):
            fields_ref[r] = flat[r * f : (r + 1) * f, :]
    pack(plan, fields_ref, packed)


def cube_root(value):
    root = jnp.exp(jnp.log(value) * (1.0 / 3.0))
    cubed = root * root * root
    better = root * (cubed + 2.0 * value) / (2.0 * cubed + value)
    return jnp.where(root > 1e-10, better, root)


def potential_kernel(ext_ref, *refs):
    *parts, out = refs
    total = parts[0][...]
    for q in parts[1:]:
        total = total + q[...]
    out[...] = ext_ref[...] - exchange_coef * cube_root(total)


def edge_kernel(plan, v_here, *refs):
    nx = len(plan.xs)
    v_there, soon, out = refs[:nx], refs[nx : 2 * nx], refs[2 * nx :]
    for ky, o in zip(plan.ys, out):
        hi = plan.above("gy", ky)
        o[0:WIDE] = v_here[pl.ds(plan.near(hi, WIDE, plan.cols), WIDE)]
        for n in range(nx):
            at = WIDE + n * (plan.v_cols + plan.corner)
            o[at : at + plan.v_cols] = v_there[n][pl.ds(plan.near(hi, plan.v_cols, plan.cols), plan.v_cols)]
            at += plan.v_cols
            base = jnp.where(hi, plan.soon_at[-1] - plan.corner, 0)
            o[at : at + plan.corner] = soon[n][pl.ds(base, plan.corner)]


def evolve_kernel(plan, final, *refs):
    nx, ny = len(plan.xs), len(plan.ys)
    refs = list(refs)
    take = lambda n: [refs.pop(0) for _ in range(n)]
    (own,) = take(1)
    soon, late, big, edge = take(nx), take(nx), take(ny), take(ny)
    (v_here,) = take(1)
    v_there = take(nx)
    if final:
        orb_ref, v_out = take(2)
    else:
        (half_ref, dens_ref) = take(2)
        packed = take(ny + 2 * nx)
    levels = take(ORDER)
    (pot,) = take(1)
    if final:
        (flat,) = take(1)
    rows, cols, f = plan.rows, plan.cols, plan.fields
    long = plan.ext_rows
    i, j = lax.axis_index("gx"), lax.axis_index("gy")
    h0 = levels[0]

    def put_potential(first, v, count):
        scaled = 24.0 * v + 90.0
        for t in range(count):
            pot[first + t] = jnp.broadcast_to(scaled[t : t + 1, :], (f, LANES))

    for c in range(cols):
        at = (WIDE + c) * long + WIDE
        h0[at : at + rows] = own[c * rows : (c + 1) * rows]
        put_potential(at, v_here[c], rows)
    for n, kx in enumerate(plan.xs):
        x_hi = plan.above("gx", kx)
        row, src = plan.beyond(x_hi, WIDE, rows), plan.at_partner(x_hi, WIDE, rows)
        for c in range(cols):
            at = (WIDE + c) * long + row
            size = plan.soon[c]
            if size:
                first = (WIDE + c) * long + plan.beyond(x_hi, size, rows)
                h0[pl.ds(first, size)] = soon[n][plan.soon_at[c] : plan.soon_at[c + 1]]
            h0[pl.ds(at + jnp.where(x_hi, size, 0), WIDE - size)] = late[n][plan.late_at[c] : plan.late_at[c + 1]]
            put_potential(at, v_there[n][c, pl.ds(src, WIDE), :], WIDE)
    for n, ky in enumerate(plan.ys):
        hi = plan.above("gy", ky)
        base = plan.beyond(hi, WIDE, cols)
        for c in range(WIDE):
            at = (base + c) * long + WIDE
            h0[pl.ds(at, rows)] = big[n][pl.ds(c * rows, rows)]
            put_potential(at, edge[n][c], rows)
        for n_x, kx in enumerate(plan.xs):
            at = WIDE + n_x * (plan.v_cols + plan.corner)
            x_hi = plan.above("gx", kx)
            row, src = plan.beyond(x_hi, WIDE, rows), plan.at_partner(x_hi, WIDE, rows)
            first = plan.beyond(hi, plan.v_cols, cols)
            for c in range(plan.v_cols):
                put_potential((first + c) * long + row, edge[n][at + c, pl.ds(src, WIDE), :], WIDE)
            at += plan.v_cols
            for d in range(1, WIDE - 1):
                size = corner_depth(d)
                there = jnp.where(hi, plan.soon_at[d - 1], plan.corner - plan.soon_at[d])
                col = jnp.where(hi, WIDE + cols + d - 1, WIDE - d)
                h0[pl.ds(col * long + plan.beyond(x_hi, size, rows), size)] = edge[n][pl.ds(at + there, size)]

    def clear_outside(h):
        for outside, col in ((j == 0, WIDE - 2), (j == plan.gy - 1, WIDE + cols)):

            @pl.when(outside)
            def _(col=col):
                for c in (col, col + 1):
                    h[c * long : (c + 1) * long] = jnp.zeros((long, f, LANES), jnp.float32)

        for outside, row in ((i == 0, WIDE - 2), (i == plan.gx - 1, WIDE + rows)):

            @pl.when(outside)
            def _(row=row):
                for c in range(plan.ext_cols):
                    h[c * long + row : c * long + row + 2] = jnp.zeros((2, f, LANES), jnp.float32)

    lane = lax.broadcasted_iota(jnp.int32, (f, LANES), 1)
    shifts = ((1, lane >= 1), (LANES - 1, lane < LANES - 1), (2, lane >= 2), (LANES - 2, lane < LANES - 2))

    def image(h, first, count, use):
        line = [h[first + t] for t in range(-2, 2)]
        for t in range(count):
            at = first + t
            line.append(h[at + 2])
            v = line[2]
            z = [jnp.where(keep, pltpu.roll(v, s, 1), 0.0) for s, keep in shifts]
            near = (line[1] + line[3]) + (h[at - long] + h[at + long]) + (z[0] + z[1])
            outer = (line[0] + line[4]) + (h[at - 2 * long] + h[at + 2 * long]) + (z[2] + z[3])
            use(at, t, (outer - 16.0 * near) + pot[at] * v)
            line.pop(0)

    clear_outside(h0)
    for k in range(1, ORDER):
        source, target = levels[k - 1], levels[k]

        def column(col, reach, source=source, target=target):
            row, count = plan.span(reach)

            def store(at, t, value):
                target[at] = value

            image(source, col * long + row, count, store)

        reach = 2 * (ORDER - k)

        @pl.loop(0, cols, unroll=divisor(cols, 6))
        def _(c, reach=reach, column=column):
            column(WIDE + c, reach)

        for m in range(1, ORDER - k + 1):
            if plan.ys:

                @pl.loop(0, 4, unroll=4)
                def _(t, m=m, reach=reach, column=column):
                    col = jnp.where(t < 2, WIDE - 2 * m, WIDE + cols + 2 * m - 4)
                    column(col + t, reach - 2 * m)

        clear_outside(target)

    sign = jnp.where(lax.broadcasted_iota(jnp.int32, (f, LANES), 0) < plan.bands, 1.0, -1.0)

    def total(s, g):
        a = [(s / 24.0) ** k for k in range(ORDER + 1)]
        even = g[0] - (a[2] / 2) * g[2] + (a[4] / 24) * g[4]
        odd = a[1] * g[1] - (a[3] / 6) * g[3]
        return even + sign * pltpu.roll(odd, plan.bands, 0)

    @pl.loop(0, cols, unroll=divisor(cols, 6))
    def _(c):
        def finish(at, t, value):
            g = [h[at] for h in levels] + [value]
            half = total(step_length / 2, g)
            cell = c * rows + t
            if final:
                flat[pl.ds(pl.multiple_of(cell * f, f), f), :] = half
            else:
                half_ref[cell] = half
                full = total(step_length, g)
                dens_ref[c, t : t + 1, :] = jnp.sum(full * full, axis=0, keepdims=True)

        image(levels[-1], (WIDE + c) * long + WIDE, rows, finish)

    if final:
        v_out[...] = v_here[...]
        for c in range(cols):
            for p in range(plan.parts):
                for b in range(plan.bands):
                    first = c * rows * f + p * plan.bands + b
                    orb_ref[p, b, c] = flat[pl.ds(first, rows, stride=f), :]
    else:
        pack(plan, half_ref, packed)


def call(kernel, outs, scratch=(), limit=8):
    spec = pl.BlockSpec(memory_space=pltpu.VMEM)
    return lambda *args: pl.pallas_call(
        kernel,
        out_shape=[jax.ShapeDtypeStruct(s, jnp.float32) for s in outs],
        in_specs=[spec] * len(args),
        out_specs=[spec] * len(outs),
        scratch_shapes=list(scratch),
        compiler_params=pltpu.CompilerParams(vmem_limit_bytes=limit << 20),
    )(*args)


def solution(mesh):
    def body(orbitals, external):
        orbitals, external = jnp.swapaxes(orbitals, 2, 3), jnp.swapaxes(external, 0, 1)
        plan = Plan(mesh, orbitals.shape)
        f, cells = plan.fields, plan.cells
        field_shape, plane = (cells, f, LANES), (plan.cols, plan.rows, LANES)
        wide = (plan.wide_cells, f, LANES)
        nx, ny = len(plan.xs), len(plan.ys)
        soon, late = plan.soon_at[-1], plan.late_at[-1]
        packed = [wide] * ny + [(soon, f, LANES)] * nx + [(late, f, LANES)] * nx

        fields, dens, *out = call(
            functools.partial(enter_kernel, plan),
            [field_shape, plane] + packed,
            [pltpu.VMEM((cells * f, LANES), jnp.float32)],
        )(orbitals)

        def gather(dens, out):
            def swap(value, **kinds):
                return plan.swap(value, **kinds)

            big = [swap(v, ky=k) for k, v in zip(plan.ys, out)]
            soon = [swap(v, kx=k) for k, v in zip(plan.xs, out[ny:])]
            late = [swap(v, kx=k) for k, v in zip(plan.xs, out[ny + nx :])]
            dens = dens + swap(dens, flip=1)
            more = [swap(dens, flip=b) for b in range(2, plan.groups, 2)]
            (v_here,) = call(potential_kernel, [plane])(external, dens, *more)
            v_there = [swap(v_here, kx=k) for k in plan.xs]
            edge = call(
                functools.partial(edge_kernel, plan), [(plan.edge_cells, f, LANES)] * ny
            )(v_here, *v_there, *soon)
            edge = [swap(v, ky=k) for k, v in zip(plan.ys, edge)]
            return [*soon, *late, *big, *edge, v_here, *v_there]

        extended = pltpu.VMEM((plan.ext_rows * plan.ext_cols, f, LANES), jnp.float32)
        scratch = [extended] * (ORDER + 1)
        arrived = gather(dens, out)
        half, dens, *out = call(
            functools.partial(evolve_kernel, plan, False), [field_shape, plane] + packed, scratch, limit=24
        )(fields, *arrived)
        arrived = gather(dens, out)
        result, potential = call(
            functools.partial(evolve_kernel, plan, True),
            [orbitals.shape, plane],
            scratch + [pltpu.VMEM((cells * f, LANES), jnp.float32)],
            limit=24,
        )(half, *arrived)
        return jnp.swapaxes(result, 2, 3), jnp.swapaxes(potential, 0, 1)

    in_specs = (P(None, "band", "gx", "gy", None), P("gx", "gy", None))
    out_specs = (P(None, "band", "gx", "gy", None), P("gx", "gy", None))
    return jax.shard_map(body, mesh=mesh, in_specs=in_specs, out_specs=out_specs, check_vma=False)
```

```python
import functools

import jax
import jax.numpy as jnp
from jax import lax
from jax.experimental import pallas as pl
from jax.experimental.pallas import tpu as pltpu
from jax.sharding import PartitionSpec as P


step_length = 0.15
exchange_coef = 0.7386
ORDER = 4
WIDE = 2 * ORDER
AXES = ("gx", "gy", "band")
LANES = 128


def corner_depth(d):
    return 2 * (ORDER - (d + 1) // 2)


def partner(kind, index, count):
    other = index ^ 1 if kind == 0 else ((index + 1) ^ 1) - 1
    return other if 0 <= other < count else None


def divisor(count, limit):
    return max(n for n in range(1, limit + 1) if count % n == 0)


class Plan:
    def __init__(self, mesh, shape):
        self.gx, self.gy, self.groups = (mesh.shape[a] for a in AXES)
        self.parts, self.bands, self.cols, self.rows, self.depth = shape
        self.fields = self.parts * self.bands
        self.cells = self.rows * self.cols
        self.xs = tuple(k for k in (0, 1) if k < self.gx - 1)
        self.ys = tuple(k for k in (0, 1) if k < self.gy - 1)
        self.ext_rows = self.rows + 2 * WIDE
        self.ext_cols = self.cols + 2 * WIDE
        self.corner = sum(corner_depth(d) for d in range(1, WIDE - 1))
        self.v_cols = WIDE // 2
        self.edge_cells = len(self.xs) * (self.corner + self.v_cols) + WIDE
        depth = [min(c + 1, self.cols - c) for c in range(self.cols)]
        self.soon = [corner_depth(d) if d < WIDE - 1 else 0 for d in depth]
        self.soon_at = [sum(self.soon[:c]) for c in range(self.cols + 1)]
        self.late_at = [c * WIDE - self.soon_at[c] for c in range(self.cols + 1)]
        self.wide_cells = WIDE * self.rows

    def pairs(self, kx=None, ky=None, flip=0):
        index = lambda i, j, b: (i * self.gy + j) * self.groups + b
        out = []
        for i in range(self.gx):
            for j in range(self.gy):
                for b in range(self.groups):
                    i2 = i if kx is None else partner(kx, i, self.gx)
                    j2 = j if ky is None else partner(ky, j, self.gy)
                    to = (i, j, b ^ 1) if i2 is None or j2 is None else (i2, j2, b ^ flip)
                    out.append((index(i, j, b), index(*to)))
        return out

    def swap(self, value, **kinds):
        return lax.ppermute(value, AXES, self.pairs(**kinds))

    def above(self, axis, kind):
        return lax.rem(lax.axis_index(axis), 2) == kind

    def near(self, hi, size, extent):
        return 0 if size == extent else jnp.where(hi, extent - size, 0)

    def beyond(self, hi, size, extent):
        return jnp.where(hi, WIDE + extent, WIDE - size)

    def at_partner(self, hi, size, extent):
        return 0 if size == extent else jnp.where(hi, 0, extent - size)

    def span(self, reach):
        if len(self.xs) == 2:
            return WIDE - reach, self.rows + 2 * reach
        if not self.xs:
            return WIDE, self.rows
        return jnp.where(self.above("gx", 0), WIDE, WIDE - reach), self.rows + reach


def pack(plan, fields_ref, out_refs):
    nx, ny = len(plan.xs), len(plan.ys)
    rows = plan.rows
    for ky, out in zip(plan.ys, out_refs[:ny]):
        base = plan.near(plan.above("gy", ky), WIDE, plan.cols)
        for c in range(WIDE):
            out[pl.ds(c * rows, rows)] = fields_ref[pl.ds((base + c) * rows, rows)]
    for kx, soon, late in zip(plan.xs, out_refs[ny : ny + nx], out_refs[ny + nx :]):
        hi = plan.above("gx", kx)
        for c, n in enumerate(plan.soon):
            if n:
                soon[plan.soon_at[c] : plan.soon_at[c + 1]] = fields_ref[pl.ds(c * rows + plan.near(hi, n, rows), n)]
            first = c * rows + jnp.where(hi, rows - WIDE, n)
            late[plan.late_at[c] : plan.late_at[c + 1]] = fields_ref[pl.ds(first, WIDE - n)]


def enter_kernel(plan, orb_ref, fields_ref, dens_ref, *rest):
    *packed, flat = rest
    f, rows = plan.fields, plan.rows
    for c in range(plan.cols):
        total = None
        for p in range(plan.parts):
            for b in range(plan.bands):
                v = orb_ref[p, b, c]
                flat[pl.ds(c * rows * f + p * plan.bands + b, rows, stride=f), :] = v
                total = v * v if total is None else total + v * v
        dens_ref[c] = total
        for r in range(c * rows, (c + 1) * rows):
            fields_ref[r] = flat[r * f : (r + 1) * f, :]
    pack(plan, fields_ref, packed)


def cube_root(value):
    root = jnp.exp(jnp.log(value) * (1.0 / 3.0))
    cubed = root * root * root
    better = root * (cubed + 2.0 * value) / (2.0 * cubed + value)
    return jnp.where(root > 1e-10, better, root)


def potential_kernel(ext_ref, *refs):
    *parts, out = refs
    total = parts[0][...]
    for q in parts[1:]:
        total = total + q[...]
    out[...] = ext_ref[...] - exchange_coef * cube_root(total)


def edge_kernel(plan, v_here, *refs):
    nx = len(plan.xs)
    v_there, soon, out = refs[:nx], refs[nx : 2 * nx], refs[2 * nx :]
    for ky, o in zip(plan.ys, out):
        hi = plan.above("gy", ky)
        o[0:WIDE] = v_here[pl.ds(plan.near(hi, WIDE, plan.cols), WIDE)]
        for n in range(nx):
            at = WIDE + n * (plan.v_cols + plan.corner)
            o[at : at + plan.v_cols] = v_there[n][pl.ds(plan.near(hi, plan.v_cols, plan.cols), plan.v_cols)]
            at += plan.v_cols
            base = jnp.where(hi, plan.soon_at[-1] - plan.corner, 0)
            o[at : at + plan.corner] = soon[n][pl.ds(base, plan.corner)]


class Steps:
    def __init__(self, plan, levels, pot):
        self.plan, self.levels, self.pot = plan, levels, pot
        self.tile = (plan.fields, LANES)
        lane = lax.broadcasted_iota(jnp.int32, self.tile, 1)
        masks = ((1, lane >= 1), (LANES - 1, lane < LANES - 1), (2, lane >= 2), (LANES - 2, lane < LANES - 2))
        self.shifts = masks

    def put_potential(self, first, v, count):
        scaled = 24.0 * v + 90.0
        for t in range(count):
            self.pot[first + t] = jnp.broadcast_to(scaled[t : t + 1, :], self.tile)

    def clear_rows(self, h):
        plan, i = self.plan, lax.axis_index("gx")
        for outside, row in ((i == 0, WIDE - 2), (i == plan.gx - 1, WIDE + plan.rows)):

            @pl.when(outside)
            def _(row=row):
                for c in range(plan.ext_cols):
                    at = c * plan.ext_rows + row
                    h[at : at + 2] = jnp.zeros((2, *self.tile), jnp.float32)

    def clear_cols(self, h):
        plan, j, long = self.plan, lax.axis_index("gy"), self.plan.ext_rows
        for outside, col in ((j == 0, WIDE - 2), (j == plan.gy - 1, WIDE + plan.cols)):

            @pl.when(outside)
            def _(col=col):
                for c in (col, col + 1):
                    h[c * long : (c + 1) * long] = jnp.zeros((long, *self.tile), jnp.float32)

    def image(self, h, first, count, use):
        long = self.plan.ext_rows
        line = [h[first + t] for t in range(-2, 2)]
        for t in range(count):
            at = first + t
            line.append(h[at + 2])
            v = line[2]
            z = [jnp.where(keep, pltpu.roll(v, s, 1), 0.0) for s, keep in self.shifts]
            near = (line[1] + line[3]) + (h[at - long] + h[at + long]) + (z[0] + z[1])
            outer = (line[0] + line[4]) + (h[at - 2 * long] + h[at + 2 * long]) + (z[2] + z[3])
            use(at, t, (outer - 16.0 * near) + self.pot[at] * v)
            line.pop(0)

    def step(self, k, first, count, spans, unroll):
        source, target = self.levels[k - 1], self.levels[k]

        def store(at, t, value):
            target[at] = value

        @pl.loop(0, count, unroll=divisor(count, unroll))
        def _(t):
            for row, size in spans:
                self.image(source, (first(t) if callable(first) else first + t) * self.plan.ext_rows + row, size, store)

    def both_sides(self, inner, m):
        plan = self.plan
        if inner:
            low, high = WIDE + 2 * m - 2, WIDE + plan.cols - 2 * m
        else:
            low, high = WIDE - 2 * m, WIDE + plan.cols + 2 * m - 2
        return lambda t: jnp.where(t < 2, low, high - 2) + t

    def own(self):
        return [(WIDE, self.plan.rows)]

    def full(self, reach):
        return [self.plan.span(reach)]

    def outside(self, reach):
        plan = self.plan
        return [(plan.beyond(plan.above("gx", kx), reach, plan.rows), reach) for kx in plan.xs] if reach else []


def inner_kernel(plan, *refs):
    nx, ny = len(plan.xs), len(plan.ys)
    refs = list(refs)
    take = lambda n: [refs.pop(0) for _ in range(n)]
    (own,) = take(1)
    soon, late, big = take(nx), take(nx), take(ny)
    (v_here,) = take(1)
    v_there = take(nx)
    levels, (pot,) = take(ORDER), take(1)
    rows, cols, long = plan.rows, plan.cols, plan.ext_rows
    steps = Steps(plan, levels, pot)
    h0 = levels[0]
    for c in range(cols):
        at = (WIDE + c) * long + WIDE
        h0[at : at + rows] = own[c * rows : (c + 1) * rows]
        steps.put_potential(at, v_here[c], rows)
    for n, kx in enumerate(plan.xs):
        x_hi = plan.above("gx", kx)
        row, src = plan.beyond(x_hi, WIDE, rows), plan.at_partner(x_hi, WIDE, rows)
        for c in range(cols):
            at, size = (WIDE + c) * long + row, plan.soon[c]
            if size:
                first = (WIDE + c) * long + plan.beyond(x_hi, size, rows)
                h0[pl.ds(first, size)] = soon[n][plan.soon_at[c] : plan.soon_at[c + 1]]
            h0[pl.ds(at + jnp.where(x_hi, size, 0), WIDE - size)] = late[n][plan.late_at[c] : plan.late_at[c + 1]]
            steps.put_potential(at, v_there[n][c, pl.ds(src, WIDE), :], WIDE)
    for n, ky in enumerate(plan.ys):
        base = plan.beyond(plan.above("gy", ky), WIDE, cols)
        for c in range(WIDE):
            h0[pl.ds((base + c) * long + WIDE, rows)] = big[n][c * rows : (c + 1) * rows]
    for h in levels:
        steps.clear_rows(h)
    steps.clear_cols(h0)
    steps.step(1, WIDE + 2, cols - 4, steps.full(6), 4)
    steps.step(1, steps.both_sides(True, 1), 4, steps.own(), 4)
    steps.step(2, WIDE + 4, cols - 8, steps.full(4), 4)
    steps.step(2, steps.both_sides(True, 2), 4, steps.own(), 4)
    steps.step(3, WIDE + 4, cols - 8, steps.own(), 4)


def evolve_kernel(plan, final, *refs):
    nx, ny = len(plan.xs), len(plan.ys)
    refs = list(refs)
    take = lambda n: [refs.pop(0) for _ in range(n)]
    take(ORDER + 1)
    edge = take(ny)
    if final:
        (v_here,) = take(1)
    levels, (pot,) = take(ORDER), take(1)
    if final:
        orb_ref, v_out, flat = take(3)
    else:
        half_ref, dens_ref = take(2)
        packed = take(ny + 2 * nx)
    rows, cols, f, long = plan.rows, plan.cols, plan.fields, plan.ext_rows
    steps = Steps(plan, levels, pot)
    h0 = levels[0]
    for n, ky in enumerate(plan.ys):
        hi = plan.above("gy", ky)
        base = plan.beyond(hi, WIDE, cols)
        for c in range(WIDE):
            steps.put_potential((base + c) * long + WIDE, edge[n][c], rows)
        for n_x, kx in enumerate(plan.xs):
            at = WIDE + n_x * (plan.v_cols + plan.corner)
            x_hi = plan.above("gx", kx)
            row, src = plan.beyond(x_hi, WIDE, rows), plan.at_partner(x_hi, WIDE, rows)
            first = plan.beyond(hi, plan.v_cols, cols)
            for c in range(plan.v_cols):
                steps.put_potential((first + c) * long + row, edge[n][at + c, pl.ds(src, WIDE), :], WIDE)
            at += plan.v_cols
            for d in range(1, WIDE - 1):
                size = corner_depth(d)
                there = jnp.where(hi, plan.soon_at[d - 1], plan.corner - plan.soon_at[d])
                col = jnp.where(hi, WIDE + cols + d - 1, WIDE - d)
                h0[pl.ds(col * long + plan.beyond(x_hi, size, rows), size)] = edge[n][pl.ds(at + there, size)]

    def clear(h):
        steps.clear_cols(h)
        if nx > 1:
            steps.clear_rows(h)

    clear(h0)
    for m in (1, 2, 3):
        steps.step(1, steps.both_sides(False, m), 4, steps.full(6 - 2 * m), 4)
    steps.step(1, steps.both_sides(True, 1), 4, steps.outside(6), 4)
    clear(levels[1])
    for m in (1, 2):
        steps.step(2, steps.both_sides(False, m), 4, steps.full(4 - 2 * m), 4)
    steps.step(2, steps.both_sides(True, 1), 4, steps.full(4), 4)
    steps.step(2, steps.both_sides(True, 2), 4, steps.outside(4), 4)
    clear(levels[2])
    steps.step(3, steps.both_sides(False, 1), 4, steps.full(0), 4)
    for m in (1, 2):
        steps.step(3, steps.both_sides(True, m), 4, steps.full(2), 4)
    steps.step(3, WIDE + 4, cols - 8, steps.outside(2), 4)
    clear(levels[3])

    sign = jnp.where(lax.broadcasted_iota(jnp.int32, (f, LANES), 0) < plan.bands, 1.0, -1.0)

    def total(s, g):
        a = [(s / 24.0) ** k for k in range(ORDER + 1)]
        even = g[0] - (a[2] / 2) * g[2] + (a[4] / 24) * g[4]
        odd = a[1] * g[1] - (a[3] / 6) * g[3]
        return even + sign * pltpu.roll(odd, plan.bands, 0)

    @pl.loop(0, cols, unroll=divisor(cols, 6))
    def _(c):
        def finish(at, t, value):
            g = [h[at] for h in levels] + [value]
            half = total(step_length / 2, g)
            cell = c * rows + t
            if final:
                flat[pl.ds(pl.multiple_of(cell * f, f), f), :] = half
            else:
                half_ref[cell] = half
                full = total(step_length, g)
                dens_ref[c, t : t + 1, :] = jnp.sum(full * full, axis=0, keepdims=True)

        steps.image(levels[-1], (WIDE + c) * long + WIDE, rows, finish)

    if final:
        v_out[...] = v_here[...]
        for c in range(cols):
            for p in range(plan.parts):
                for b in range(plan.bands):
                    first = c * rows * f + p * plan.bands + b
                    orb_ref[p, b, c] = flat[pl.ds(first, rows, stride=f), :]
    else:
        pack(plan, half_ref, packed)


def call(kernel, outs, scratch=(), limit=8, alias=0):
    spec = pl.BlockSpec(memory_space=pltpu.VMEM)
    return lambda *args: pl.pallas_call(
        kernel,
        out_shape=[jax.ShapeDtypeStruct(s, jnp.float32) for s in outs],
        in_specs=[spec] * len(args),
        out_specs=[spec] * len(outs),
        scratch_shapes=list(scratch),
        input_output_aliases={n: n for n in range(alias)},
        compiler_params=pltpu.CompilerParams(vmem_limit_bytes=limit << 20),
    )(*args)


def solution(mesh):
    def body(orbitals, external):
        orbitals, external = jnp.swapaxes(orbitals, 2, 3), jnp.swapaxes(external, 0, 1)
        plan = Plan(mesh, orbitals.shape)
        f, cells = plan.fields, plan.cells
        field_shape, plane = (cells, f, LANES), (plan.cols, plan.rows, LANES)
        wide = (plan.wide_cells, f, LANES)
        nx, ny = len(plan.xs), len(plan.ys)
        soon, late = plan.soon_at[-1], plan.late_at[-1]
        packed = [wide] * ny + [(soon, f, LANES)] * nx + [(late, f, LANES)] * nx

        fields, dens, *out = call(
            functools.partial(enter_kernel, plan),
            [field_shape, plane] + packed,
            [pltpu.VMEM((cells * f, LANES), jnp.float32)],
        )(orbitals)

        extended = (plan.ext_rows * plan.ext_cols, f, LANES)

        def load(ext_ref, out_ref):
            out_ref[...] = ext_ref[...]

        (external,) = call(load, [plane])(external)

        def gather(fields, dens, out):
            def swap(value, **kinds):
                return plan.swap(value, **kinds)

            big = [swap(v, ky=k) for k, v in zip(plan.ys, out)]
            soon = [swap(v, kx=k) for k, v in zip(plan.xs, out[ny:])]
            late = [swap(v, kx=k) for k, v in zip(plan.xs, out[ny + nx :])]
            dens = dens + swap(dens, flip=1)
            more = [swap(dens, flip=b) for b in range(2, plan.groups, 2)]
            (v_here,) = call(potential_kernel, [plane])(external, dens, *more)
            v_there = [swap(v_here, kx=k) for k in plan.xs]
            edge = call(
                functools.partial(edge_kernel, plan), [(plan.edge_cells, f, LANES)] * ny
            )(v_here, *v_there, *soon)
            edge = [swap(v, ky=k) for k, v in zip(plan.ys, edge)]
            inside = call(
                functools.partial(inner_kernel, plan), [extended] * (ORDER + 1), limit=4
            )(fields, *soon, *late, *big, v_here, *v_there)
            return [*inside, *edge], v_here

        blocks = [extended] * (ORDER + 1)
        arrived, _ = gather(fields, dens, out)
        half, dens, *out = call(
            functools.partial(evolve_kernel, plan, False),
            blocks + [field_shape, plane] + packed,
            limit=4,
            alias=len(blocks),
        )(*arrived)[len(blocks) :]
        arrived, v_here = gather(half, dens, out)
        result, potential = call(
            functools.partial(evolve_kernel, plan, True),
            blocks + [orbitals.shape, plane],
            [pltpu.VMEM((cells * f, LANES), jnp.float32)],
            limit=4,
            alias=len(blocks),
        )(*arrived, v_here)[len(blocks) :]
        return jnp.swapaxes(result, 2, 3), jnp.swapaxes(potential, 0, 1)

    in_specs = (P(None, "band", "gx", "gy", None), P("gx", "gy", None))
    out_specs = (P(None, "band", "gx", "gy", None), P("gx", "gy", None))
    return jax.shard_map(body, mesh=mesh, in_specs=in_specs, out_specs=out_specs, check_vma=False)
```

```python
import functools

import jax
import jax.numpy as jnp
from jax import lax
from jax.experimental import pallas as pl
from jax.experimental.pallas import tpu as pltpu
from jax.sharding import PartitionSpec as P


step_length = 0.15
exchange_coef = 0.7386
ORDER = 4
WIDE = 2 * ORDER
AXES = ("gx", "gy", "band")
LANES = 128


def corner_depth(d):
    return 2 * (ORDER - (d + 1) // 2)


def partner(kind, index, count):
    other = index ^ 1 if kind == 0 else ((index + 1) ^ 1) - 1
    return other if 0 <= other < count else None


def divisor(count, limit):
    return max(n for n in range(1, limit + 1) if count % n == 0)


class Plan:
    def __init__(self, mesh, shape):
        self.gx, self.gy, self.groups = (mesh.shape[a] for a in AXES)
        self.parts, self.bands, self.cols, self.rows, self.depth = shape
        self.fields = self.parts * self.bands
        self.cells = self.rows * self.cols
        self.xs = tuple(k for k in (0, 1) if k < self.gx - 1)
        self.ys = tuple(k for k in (0, 1) if k < self.gy - 1)
        self.ext_rows = self.rows + 2 * WIDE
        self.ext_cols = self.cols + 2 * WIDE
        self.corner = sum(corner_depth(d) for d in range(1, WIDE - 1))
        self.v_cols = WIDE // 2
        self.edge_cells = len(self.xs) * (self.corner + self.v_cols) + WIDE
        depth = [min(c + 1, self.cols - c) for c in range(self.cols)]
        self.soon = [corner_depth(d) if d < WIDE - 1 else 0 for d in depth]
        self.soon_at = [sum(self.soon[:c]) for c in range(self.cols + 1)]
        self.late_at = [c * WIDE - self.soon_at[c] for c in range(self.cols + 1)]
        self.wide_cells = WIDE * self.rows

    def pairs(self, kx=None, ky=None, flip=0):
        index = lambda i, j, b: (i * self.gy + j) * self.groups + b
        out = []
        for i in range(self.gx):
            for j in range(self.gy):
                for b in range(self.groups):
                    i2 = i if kx is None else partner(kx, i, self.gx)
                    j2 = j if ky is None else partner(ky, j, self.gy)
                    to = (i, j, b ^ 1) if i2 is None or j2 is None else (i2, j2, b ^ flip)
                    out.append((index(i, j, b), index(*to)))
        return out

    def swap(self, value, **kinds):
        return lax.ppermute(value, AXES, self.pairs(**kinds))

    def above(self, axis, kind):
        return lax.rem(lax.axis_index(axis), 2) == kind

    def near(self, hi, size, extent):
        return 0 if size == extent else jnp.where(hi, extent - size, 0)

    def beyond(self, hi, size, extent):
        return jnp.where(hi, WIDE + extent, WIDE - size)

    def at_partner(self, hi, size, extent):
        return 0 if size == extent else jnp.where(hi, 0, extent - size)

    def span(self, reach):
        if len(self.xs) == 2:
            return WIDE - reach, self.rows + 2 * reach
        if not self.xs:
            return WIDE, self.rows
        return jnp.where(self.above("gx", 0), WIDE, WIDE - reach), self.rows + reach


def pack(plan, fields_ref, out_refs):
    nx, ny = len(plan.xs), len(plan.ys)
    rows = plan.rows
    for ky, out in zip(plan.ys, out_refs[:ny]):
        base = plan.near(plan.above("gy", ky), WIDE, plan.cols)
        for c in range(WIDE):
            out[pl.ds(c * rows, rows)] = fields_ref[pl.ds((base + c) * rows, rows)]
    for kx, soon, late in zip(plan.xs, out_refs[ny : ny + nx], out_refs[ny + nx :]):
        hi = plan.above("gx", kx)
        for c, n in enumerate(plan.soon):
            if n:
                soon[plan.soon_at[c] : plan.soon_at[c + 1]] = fields_ref[pl.ds(c * rows + plan.near(hi, n, rows), n)]
            first = c * rows + jnp.where(hi, rows - WIDE, n)
            late[plan.late_at[c] : plan.late_at[c + 1]] = fields_ref[pl.ds(first, WIDE - n)]


def enter_kernel(plan, orb_ref, fields_ref, dens_ref, *rest):
    *packed, flat = rest
    f, rows = plan.fields, plan.rows
    for c in range(plan.cols):
        total = None
        for p in range(plan.parts):
            for b in range(plan.bands):
                v = orb_ref[p, b, c]
                flat[pl.ds(c * rows * f + p * plan.bands + b, rows, stride=f), :] = v
                total = v * v if total is None else total + v * v
        dens_ref[c] = total
        for r in range(c * rows, (c + 1) * rows):
            fields_ref[r] = flat[r * f : (r + 1) * f, :]
    pack(plan, fields_ref, packed)


def cube_root(value):
    root = jnp.exp(jnp.log(value) * (1.0 / 3.0))
    cubed = root * root * root
    better = root * (cubed + 2.0 * value) / (2.0 * cubed + value)
    return jnp.where(root > 1e-10, better, root)


def potential_kernel(ext_ref, *refs):
    *parts, out = refs
    total = parts[0][...]
    for q in parts[1:]:
        total = total + q[...]
    out[...] = ext_ref[...] - exchange_coef * cube_root(total)


def edge_kernel(plan, v_here, *refs):
    nx = len(plan.xs)
    v_there, soon, out = refs[:nx], refs[nx : 2 * nx], refs[2 * nx :]
    for ky, o in zip(plan.ys, out):
        hi = plan.above("gy", ky)
        o[0:WIDE] = v_here[pl.ds(plan.near(hi, WIDE, plan.cols), WIDE)]
        for n in range(nx):
            at = WIDE + n * (plan.v_cols + plan.corner)
            o[at : at + plan.v_cols] = v_there[n][pl.ds(plan.near(hi, plan.v_cols, plan.cols), plan.v_cols)]
            at += plan.v_cols
            base = jnp.where(hi, plan.soon_at[-1] - plan.corner, 0)
            o[at : at + plan.corner] = soon[n][pl.ds(base, plan.corner)]


class Steps:
    def __init__(self, plan, levels, pot):
        self.plan, self.levels, self.pot = plan, levels, pot
        self.tile = (plan.fields, LANES)
        apart = lax.broadcasted_iota(jnp.int32, (LANES, LANES), 0) - lax.broadcasted_iota(jnp.int32, (LANES, LANES), 1)
        apart = jnp.abs(apart)
        weights = jnp.where(apart == 1, -16.0, jnp.where(apart == 2, 1.0, 0.0))
        self.weights = weights.astype(jnp.bfloat16)

    def along_z(self, cells):
        flat = cells.reshape(-1, LANES)
        high = flat.astype(jnp.bfloat16)
        low = (flat - high.astype(jnp.float32)).astype(jnp.bfloat16)
        times = lambda v: jnp.dot(v, self.weights, preferred_element_type=jnp.float32)
        return (times(high) + times(low)).reshape(cells.shape)

    def put_potential(self, first, v, count):
        scaled = 24.0 * v + 90.0
        for t in range(count):
            self.pot[first + t] = jnp.broadcast_to(scaled[t : t + 1, :], self.tile)

    def clear_rows(self, h):
        plan, i = self.plan, lax.axis_index("gx")
        for outside, row in ((i == 0, WIDE - 2), (i == plan.gx - 1, WIDE + plan.rows)):

            @pl.when(outside)
            def _(row=row):
                for c in range(plan.ext_cols):
                    at = c * plan.ext_rows + row
                    h[at : at + 2] = jnp.zeros((2, *self.tile), jnp.float32)

    def clear_cols(self, h):
        plan, j, long = self.plan, lax.axis_index("gy"), self.plan.ext_rows
        for outside, col in ((j == 0, WIDE - 2), (j == plan.gy - 1, WIDE + plan.cols)):

            @pl.when(outside)
            def _(col=col):
                for c in (col, col + 1):
                    h[c * long : (c + 1) * long] = jnp.zeros((long, *self.tile), jnp.float32)

    def image(self, h, first, count, use):
        long = self.plan.ext_rows
        line = [h[first + t] for t in range(-2, 2)]
        z = self.along_z(h[pl.ds(first, count)])
        for t in range(count):
            at = first + t
            line.append(h[at + 2])
            v = line[2]
            near = (line[1] + line[3]) + (h[at - long] + h[at + long])
            outer = (line[0] + line[4]) + (h[at - 2 * long] + h[at + 2 * long])
            use(at, t, (outer - 16.0 * near) + (z[t] + self.pot[at] * v))
            line.pop(0)

    def step(self, k, first, count, spans, unroll):
        source, target = self.levels[k - 1], self.levels[k]

        def store(at, t, value):
            target[at] = value

        @pl.loop(0, count, unroll=divisor(count, unroll))
        def _(t):
            for row, size in spans:
                self.image(source, (first(t) if callable(first) else first + t) * self.plan.ext_rows + row, size, store)

    def both_sides(self, inner, m):
        plan = self.plan
        if inner:
            low, high = WIDE + 2 * m - 2, WIDE + plan.cols - 2 * m
        else:
            low, high = WIDE - 2 * m, WIDE + plan.cols + 2 * m - 2
        return lambda t: jnp.where(t < 2, low, high - 2) + t

    def own(self):
        return [(WIDE, self.plan.rows)]

    def full(self, reach):
        return [self.plan.span(reach)]

    def outside(self, reach):
        plan = self.plan
        return [(plan.beyond(plan.above("gx", kx), reach, plan.rows), reach) for kx in plan.xs] if reach else []


def inner_kernel(plan, *refs):
    nx, ny = len(plan.xs), len(plan.ys)
    refs = list(refs)
    take = lambda n: [refs.pop(0) for _ in range(n)]
    (own,) = take(1)
    soon, late, big = take(nx), take(nx), take(ny)
    (v_here,) = take(1)
    v_there = take(nx)
    levels, (pot,) = take(ORDER), take(1)
    rows, cols, long = plan.rows, plan.cols, plan.ext_rows
    steps = Steps(plan, levels, pot)
    h0 = levels[0]
    for c in range(cols):
        at = (WIDE + c) * long + WIDE
        h0[at : at + rows] = own[c * rows : (c + 1) * rows]
        steps.put_potential(at, v_here[c], rows)
    for n, kx in enumerate(plan.xs):
        x_hi = plan.above("gx", kx)
        row, src = plan.beyond(x_hi, WIDE, rows), plan.at_partner(x_hi, WIDE, rows)
        for c in range(cols):
            at, size = (WIDE + c) * long + row, plan.soon[c]
            if size:
                first = (WIDE + c) * long + plan.beyond(x_hi, size, rows)
                h0[pl.ds(first, size)] = soon[n][plan.soon_at[c] : plan.soon_at[c + 1]]
            h0[pl.ds(at + jnp.where(x_hi, size, 0), WIDE - size)] = late[n][plan.late_at[c] : plan.late_at[c + 1]]
            steps.put_potential(at, v_there[n][c, pl.ds(src, WIDE), :], WIDE)
    for n, ky in enumerate(plan.ys):
        base = plan.beyond(plan.above("gy", ky), WIDE, cols)
        for c in range(WIDE):
            h0[pl.ds((base + c) * long + WIDE, rows)] = big[n][c * rows : (c + 1) * rows]
    for h in levels:
        steps.clear_rows(h)
    steps.clear_cols(h0)
    steps.step(1, WIDE + 2, cols - 4, steps.full(6), 4)
    steps.step(1, steps.both_sides(True, 1), 4, steps.own(), 4)
    steps.step(2, WIDE + 4, cols - 8, steps.full(4), 4)
    steps.step(2, steps.both_sides(True, 2), 4, steps.own(), 4)
    steps.step(3, WIDE + 4, cols - 8, steps.own(), 4)


def evolve_kernel(plan, final, *refs):
    nx, ny = len(plan.xs), len(plan.ys)
    refs = list(refs)
    take = lambda n: [refs.pop(0) for _ in range(n)]
    take(ORDER + 1)
    edge = take(ny)
    if final:
        (v_here,) = take(1)
    levels, (pot,) = take(ORDER), take(1)
    if final:
        orb_ref, v_out, flat = take(3)
    else:
        half_ref, dens_ref = take(2)
        packed = take(ny + 2 * nx)
    rows, cols, f, long = plan.rows, plan.cols, plan.fields, plan.ext_rows
    steps = Steps(plan, levels, pot)
    h0 = levels[0]
    for n, ky in enumerate(plan.ys):
        hi = plan.above("gy", ky)
        base = plan.beyond(hi, WIDE, cols)
        for c in range(WIDE):
            steps.put_potential((base + c) * long + WIDE, edge[n][c], rows)
        for n_x, kx in enumerate(plan.xs):
            at = WIDE + n_x * (plan.v_cols + plan.corner)
            x_hi = plan.above("gx", kx)
            row, src = plan.beyond(x_hi, WIDE, rows), plan.at_partner(x_hi, WIDE, rows)
            first = plan.beyond(hi, plan.v_cols, cols)
            for c in range(plan.v_cols):
                steps.put_potential((first + c) * long + row, edge[n][at + c, pl.ds(src, WIDE), :], WIDE)
            at += plan.v_cols
            for d in range(1, WIDE - 1):
                size = corner_depth(d)
                there = jnp.where(hi, plan.soon_at[d - 1], plan.corner - plan.soon_at[d])
                col = jnp.where(hi, WIDE + cols + d - 1, WIDE - d)
                h0[pl.ds(col * long + plan.beyond(x_hi, size, rows), size)] = edge[n][pl.ds(at + there, size)]

    def clear(h):
        steps.clear_cols(h)
        if nx > 1:
            steps.clear_rows(h)

    clear(h0)
    for m in (1, 2, 3):
        steps.step(1, steps.both_sides(False, m), 4, steps.full(6 - 2 * m), 4)
    steps.step(1, steps.both_sides(True, 1), 4, steps.outside(6), 4)
    clear(levels[1])
    for m in (1, 2):
        steps.step(2, steps.both_sides(False, m), 4, steps.full(4 - 2 * m), 4)
    steps.step(2, steps.both_sides(True, 1), 4, steps.full(4), 4)
    steps.step(2, steps.both_sides(True, 2), 4, steps.outside(4), 4)
    clear(levels[2])
    steps.step(3, steps.both_sides(False, 1), 4, steps.full(0), 4)
    for m in (1, 2):
        steps.step(3, steps.both_sides(True, m), 4, steps.full(2), 4)
    steps.step(3, WIDE + 4, cols - 8, steps.outside(2), 4)
    clear(levels[3])

    sign = jnp.where(lax.broadcasted_iota(jnp.int32, (f, LANES), 0) < plan.bands, 1.0, -1.0)

    def total(s, g):
        a = [(s / 24.0) ** k for k in range(ORDER + 1)]
        even = g[0] - (a[2] / 2) * g[2] + (a[4] / 24) * g[4]
        odd = a[1] * g[1] - (a[3] / 6) * g[3]
        return even + sign * pltpu.roll(odd, plan.bands, 0)

    @pl.loop(0, cols, unroll=divisor(cols, 6))
    def _(c):
        def finish(at, t, value):
            g = [h[at] for h in levels] + [value]
            half = total(step_length / 2, g)
            cell = c * rows + t
            if final:
                flat[pl.ds(pl.multiple_of(cell * f, f), f), :] = half
            else:
                half_ref[cell] = half
                full = total(step_length, g)
                dens_ref[c, t : t + 1, :] = jnp.sum(full * full, axis=0, keepdims=True)

        steps.image(levels[-1], (WIDE + c) * long + WIDE, rows, finish)

    if final:
        v_out[...] = v_here[...]
        for c in range(cols):
            for p in range(plan.parts):
                for b in range(plan.bands):
                    first = c * rows * f + p * plan.bands + b
                    orb_ref[p, b, c] = flat[pl.ds(first, rows, stride=f), :]
    else:
        pack(plan, half_ref, packed)


def call(kernel, outs, scratch=(), limit=8, alias=0):
    spec = pl.BlockSpec(memory_space=pltpu.VMEM)
    return lambda *args: pl.pallas_call(
        kernel,
        out_shape=[jax.ShapeDtypeStruct(s, jnp.float32) for s in outs],
        in_specs=[spec] * len(args),
        out_specs=[spec] * len(outs),
        scratch_shapes=list(scratch),
        input_output_aliases={n: n for n in range(alias)},
        compiler_params=pltpu.CompilerParams(vmem_limit_bytes=limit << 20),
    )(*args)


def solution(mesh):
    def body(orbitals, external):
        orbitals, external = jnp.swapaxes(orbitals, 2, 3), jnp.swapaxes(external, 0, 1)
        plan = Plan(mesh, orbitals.shape)
        f, cells = plan.fields, plan.cells
        field_shape, plane = (cells, f, LANES), (plan.cols, plan.rows, LANES)
        wide = (plan.wide_cells, f, LANES)
        nx, ny = len(plan.xs), len(plan.ys)
        soon, late = plan.soon_at[-1], plan.late_at[-1]
        packed = [wide] * ny + [(soon, f, LANES)] * nx + [(late, f, LANES)] * nx

        fields, dens, *out = call(
            functools.partial(enter_kernel, plan),
            [field_shape, plane] + packed,
            [pltpu.VMEM((cells * f, LANES), jnp.float32)],
        )(orbitals)

        extended = (plan.ext_rows * plan.ext_cols, f, LANES)

        def load(ext_ref, out_ref):
            out_ref[...] = ext_ref[...]

        (external,) = call(load, [plane])(external)

        def gather(fields, dens, out):
            def swap(value, **kinds):
                return plan.swap(value, **kinds)

            big = [swap(v, ky=k) for k, v in zip(plan.ys, out)]
            soon = [swap(v, kx=k) for k, v in zip(plan.xs, out[ny:])]
            late = [swap(v, kx=k) for k, v in zip(plan.xs, out[ny + nx :])]
            dens = dens + swap(dens, flip=1)
            more = [swap(dens, flip=b) for b in range(2, plan.groups, 2)]
            (v_here,) = call(potential_kernel, [plane])(external, dens, *more)
            v_there = [swap(v_here, kx=k) for k in plan.xs]
            edge = call(
                functools.partial(edge_kernel, plan), [(plan.edge_cells, f, LANES)] * ny
            )(v_here, *v_there, *soon)
            edge = [swap(v, ky=k) for k, v in zip(plan.ys, edge)]
            inside = call(
                functools.partial(inner_kernel, plan), [extended] * (ORDER + 1), limit=4
            )(fields, *soon, *late, *big, v_here, *v_there)
            return [*inside, *edge], v_here

        blocks = [extended] * (ORDER + 1)
        arrived, _ = gather(fields, dens, out)
        half, dens, *out = call(
            functools.partial(evolve_kernel, plan, False),
            blocks + [field_shape, plane] + packed,
            limit=4,
            alias=len(blocks),
        )(*arrived)[len(blocks) :]
        arrived, v_here = gather(half, dens, out)
        result, potential = call(
            functools.partial(evolve_kernel, plan, True),
            blocks + [orbitals.shape, plane],
            [pltpu.VMEM((cells * f, LANES), jnp.float32)],
            limit=4,
            alias=len(blocks),
        )(*arrived, v_here)[len(blocks) :]
        return jnp.swapaxes(result, 2, 3), jnp.swapaxes(potential, 0, 1)

    in_specs = (P(None, "band", "gx", "gy", None), P("gx", "gy", None))
    out_specs = (P(None, "band", "gx", "gy", None), P("gx", "gy", None))
    return jax.shard_map(body, mesh=mesh, in_specs=in_specs, out_specs=out_specs, check_vma=False)
```

```python
import functools

import jax
import jax.numpy as jnp
from jax import lax
from jax.experimental import pallas as pl
from jax.experimental.pallas import tpu as pltpu
from jax.sharding import PartitionSpec as P


step_length = 0.15
exchange_coef = 0.7386
ORDER = 4
WIDE = 2 * ORDER
AXES = ("gx", "gy", "band")
LANES = 128


def corner_depth(d):
    return 2 * (ORDER - (d + 1) // 2)


def partner(kind, index, count):
    other = index ^ 1 if kind == 0 else ((index + 1) ^ 1) - 1
    return other if 0 <= other < count else None


def divisor(count, limit):
    return max(n for n in range(1, limit + 1) if count % n == 0)


class Plan:
    def __init__(self, mesh, shape):
        self.gx, self.gy, self.groups = (mesh.shape[a] for a in AXES)
        self.parts, self.bands, self.cols, self.rows, self.depth = shape
        self.fields = self.parts * self.bands
        self.cells = self.rows * self.cols
        self.xs = tuple(k for k in (0, 1) if k < self.gx - 1)
        self.ys = tuple(k for k in (0, 1) if k < self.gy - 1)
        self.ext_rows = self.rows + 2 * WIDE
        self.ext_cols = self.cols + 2 * WIDE
        self.corner = sum(corner_depth(d) for d in range(1, WIDE - 1))
        self.v_cols = WIDE // 2
        self.edge_cells = len(self.xs) * (self.corner + self.v_cols) + WIDE - 2
        depth = [min(c + 1, self.cols - c) for c in range(self.cols)]
        self.soon = [corner_depth(d) if d < WIDE - 1 else 0 for d in depth]
        self.soon_at = [sum(self.soon[:c]) for c in range(self.cols + 1)]
        self.late_at = [c * WIDE - self.soon_at[c] for c in range(self.cols + 1)]
        self.wide_cells = WIDE * self.rows

    def pairs(self, kx=None, ky=None, flip=0):
        index = lambda i, j, b: (i * self.gy + j) * self.groups + b
        out = []
        for i in range(self.gx):
            for j in range(self.gy):
                for b in range(self.groups):
                    i2 = i if kx is None else partner(kx, i, self.gx)
                    j2 = j if ky is None else partner(ky, j, self.gy)
                    to = (i, j, b ^ 1) if i2 is None or j2 is None else (i2, j2, b ^ flip)
                    out.append((index(i, j, b), index(*to)))
        return out

    def swap(self, value, **kinds):
        return lax.ppermute(value, AXES, self.pairs(**kinds))

    def above(self, axis, kind):
        return lax.rem(lax.axis_index(axis), 2) == kind

    def near(self, hi, size, extent):
        return 0 if size == extent else jnp.where(hi, extent - size, 0)

    def beyond(self, hi, size, extent):
        return jnp.where(hi, WIDE + extent, WIDE - size)

    def at_partner(self, hi, size, extent):
        return 0 if size == extent else jnp.where(hi, 0, extent - size)

    def span(self, reach):
        if len(self.xs) == 2:
            return WIDE - reach, self.rows + 2 * reach
        if not self.xs:
            return WIDE, self.rows
        return jnp.where(self.above("gx", 0), WIDE, WIDE - reach), self.rows + reach


def pack(plan, fields_ref, out_refs):
    nx, ny = len(plan.xs), len(plan.ys)
    rows = plan.rows
    for ky, out in zip(plan.ys, out_refs[:ny]):
        base = plan.near(plan.above("gy", ky), WIDE, plan.cols)
        for c in range(WIDE):
            out[pl.ds(c * rows, rows)] = fields_ref[pl.ds((base + c) * rows, rows)]
    for kx, soon, late in zip(plan.xs, out_refs[ny : ny + nx], out_refs[ny + nx :]):
        hi = plan.above("gx", kx)
        for c, n in enumerate(plan.soon):
            if n:
                soon[plan.soon_at[c] : plan.soon_at[c + 1]] = fields_ref[pl.ds(c * rows + plan.near(hi, n, rows), n)]
            first = c * rows + jnp.where(hi, rows - WIDE, n)
            late[plan.late_at[c] : plan.late_at[c + 1]] = fields_ref[pl.ds(first, WIDE - n)]


def enter_kernel(plan, orb_ref, fields_ref, dens_ref, *rest):
    *packed, flat = rest
    f, rows = plan.fields, plan.rows
    for c in range(plan.cols):
        total = None
        for p in range(plan.parts):
            for b in range(plan.bands):
                v = orb_ref[p, b, c]
                flat[pl.ds(c * rows * f + p * plan.bands + b, rows, stride=f), :] = v
                total = v * v if total is None else total + v * v
        dens_ref[c] = total
        for r in range(c * rows, (c + 1) * rows):
            fields_ref[r] = flat[r * f : (r + 1) * f, :]
    pack(plan, fields_ref, packed)


def cube_root(value):
    root = jnp.exp(jnp.log(value) * (1.0 / 3.0))
    cubed = root * root * root
    better = root * (cubed + 2.0 * value) / (2.0 * cubed + value)
    return jnp.where(root > 1e-10, better, root)


def potential_kernel(ext_ref, *refs):
    *parts, out = refs
    total = parts[0][...]
    for q in parts[1:]:
        total = total + q[...]
    out[...] = ext_ref[...] - exchange_coef * cube_root(total)


def edge_kernel(plan, v_here, *refs):
    nx = len(plan.xs)
    v_there, soon, out = refs[:nx], refs[nx : 2 * nx], refs[2 * nx :]
    for ky, o in zip(plan.ys, out):
        hi = plan.above("gy", ky)
        o[0 : WIDE - 2] = v_here[pl.ds(plan.near(hi, WIDE - 2, plan.cols), WIDE - 2)]
        for n in range(nx):
            at = WIDE - 2 + n * (plan.v_cols + plan.corner)
            o[at : at + plan.v_cols] = v_there[n][pl.ds(plan.near(hi, plan.v_cols, plan.cols), plan.v_cols)]
            at += plan.v_cols
            base = jnp.where(hi, plan.soon_at[-1] - plan.corner, 0)
            o[at : at + plan.corner] = soon[n][pl.ds(base, plan.corner)]


class Steps:
    def __init__(self, plan, levels, pot):
        self.plan, self.levels, self.pot = plan, levels, pot
        self.tile = (plan.fields, LANES)
        apart = lax.broadcasted_iota(jnp.int32, (LANES, LANES), 0) - lax.broadcasted_iota(jnp.int32, (LANES, LANES), 1)
        apart = jnp.abs(apart)
        weights = jnp.where(apart == 1, -16.0, jnp.where(apart == 2, 1.0, 0.0))
        self.weights = jnp.concatenate([weights, weights], axis=0).astype(jnp.bfloat16)

    def along_z(self, cells):
        flat = cells.reshape(-1, LANES)
        high = flat.astype(jnp.bfloat16)
        low = (flat - high.astype(jnp.float32)).astype(jnp.bfloat16)
        both = jnp.concatenate([high, low], axis=1)
        return jnp.dot(both, self.weights, preferred_element_type=jnp.float32).reshape(cells.shape)

    def put_potential(self, first, v, count):
        scaled = 24.0 * v + 90.0
        for t in range(count):
            self.pot[first + t] = jnp.broadcast_to(scaled[t : t + 1, :], self.tile)

    def clear_rows(self, h):
        plan, i = self.plan, lax.axis_index("gx")
        for outside, row in ((i == 0, WIDE - 2), (i == plan.gx - 1, WIDE + plan.rows)):

            @pl.when(outside)
            def _(row=row):
                for c in range(plan.ext_cols):
                    at = c * plan.ext_rows + row
                    h[at : at + 2] = jnp.zeros((2, *self.tile), jnp.float32)

    def clear_cols(self, h):
        plan, j, long = self.plan, lax.axis_index("gy"), self.plan.ext_rows
        for outside, col in ((j == 0, WIDE - 2), (j == plan.gy - 1, WIDE + plan.cols)):

            @pl.when(outside)
            def _(col=col):
                for c in (col, col + 1):
                    h[c * long : (c + 1) * long] = jnp.zeros((long, *self.tile), jnp.float32)

    def image(self, h, first, count, use):
        long = self.plan.ext_rows
        line = [h[first + t] for t in range(-2, 2)]
        z = self.along_z(h[pl.ds(first, count)])
        for t in range(count):
            at = first + t
            line.append(h[at + 2])
            v = line[2]
            near = (line[1] + line[3]) + (h[at - long] + h[at + long])
            outer = (line[0] + line[4]) + (h[at - 2 * long] + h[at + 2 * long])
            use(at, t, (outer - 16.0 * near) + (z[t] + self.pot[at] * v))
            line.pop(0)

    def step(self, k, first, count, spans, unroll):
        source, target = self.levels[k - 1], self.levels[k]

        def store(at, t, value):
            target[at] = value

        @pl.loop(0, count, unroll=divisor(count, unroll))
        def _(t):
            for row, size in spans:
                self.image(source, (first(t) if callable(first) else first + t) * self.plan.ext_rows + row, size, store)

    def both_sides(self, inner, m):
        plan = self.plan
        if inner:
            low, high = WIDE + 2 * m - 2, WIDE + plan.cols - 2 * m
        else:
            low, high = WIDE - 2 * m, WIDE + plan.cols + 2 * m - 2
        return lambda t: jnp.where(t < 2, low, high - 2) + t

    def own(self):
        return [(WIDE, self.plan.rows)]

    def full(self, reach):
        return [self.plan.span(reach)]

    def outside(self, reach):
        plan = self.plan
        return [(plan.beyond(plan.above("gx", kx), reach, plan.rows), reach) for kx in plan.xs] if reach else []


def inner_kernel(plan, *refs):
    nx, ny = len(plan.xs), len(plan.ys)
    refs = list(refs)
    take = lambda n: [refs.pop(0) for _ in range(n)]
    (own,) = take(1)
    soon, late, big = take(nx), take(nx), take(ny)
    (v_here,) = take(1)
    v_there = take(nx)
    levels, (pot,) = take(ORDER), take(1)
    rows, cols, long = plan.rows, plan.cols, plan.ext_rows
    steps = Steps(plan, levels, pot)
    h0 = levels[0]
    for c in range(cols):
        at = (WIDE + c) * long + WIDE
        h0[at : at + rows] = own[c * rows : (c + 1) * rows]
        steps.put_potential(at, v_here[c], rows)
    for n, kx in enumerate(plan.xs):
        x_hi = plan.above("gx", kx)
        row, src = plan.beyond(x_hi, WIDE, rows), plan.at_partner(x_hi, WIDE, rows)
        for c in range(cols):
            at, size = (WIDE + c) * long + row, plan.soon[c]
            if size:
                first = (WIDE + c) * long + plan.beyond(x_hi, size, rows)
                h0[pl.ds(first, size)] = soon[n][plan.soon_at[c] : plan.soon_at[c + 1]]
            h0[pl.ds(at + jnp.where(x_hi, size, 0), WIDE - size)] = late[n][plan.late_at[c] : plan.late_at[c + 1]]
            steps.put_potential(at, v_there[n][c, pl.ds(src, WIDE), :], WIDE)
    for n, ky in enumerate(plan.ys):
        base = plan.beyond(plan.above("gy", ky), WIDE, cols)
        for c in range(WIDE):
            h0[pl.ds((base + c) * long + WIDE, rows)] = big[n][c * rows : (c + 1) * rows]
    for h in levels:
        steps.clear_rows(h)
    steps.clear_cols(h0)
    steps.step(1, WIDE + 2, cols - 4, steps.full(6), 4)
    steps.step(1, steps.both_sides(True, 1), 4, steps.own(), 4)
    steps.step(2, WIDE + 4, cols - 8, steps.full(4), 4)
    steps.step(2, steps.both_sides(True, 2), 4, steps.own(), 4)
    steps.step(3, WIDE + 4, cols - 8, steps.own(), 4)


def evolve_kernel(plan, final, *refs):
    nx, ny = len(plan.xs), len(plan.ys)
    refs = list(refs)
    take = lambda n: [refs.pop(0) for _ in range(n)]
    take(ORDER + 1)
    edge = take(ny)
    if final:
        (v_here,) = take(1)
    levels, (pot,) = take(ORDER), take(1)
    if final:
        orb_ref, v_out, flat = take(3)
    else:
        half_ref, dens_ref = take(2)
        packed = take(ny + 2 * nx)
        (flat,) = take(1)
    rows, cols, f, long = plan.rows, plan.cols, plan.fields, plan.ext_rows
    steps = Steps(plan, levels, pot)
    h0 = levels[0]
    for n, ky in enumerate(plan.ys):
        hi = plan.above("gy", ky)
        base = plan.beyond(hi, WIDE - 2, cols)
        for c in range(WIDE - 2):
            steps.put_potential((base + c) * long + WIDE, edge[n][c], rows)
        for n_x, kx in enumerate(plan.xs):
            at = WIDE - 2 + n_x * (plan.v_cols + plan.corner)
            x_hi = plan.above("gx", kx)
            row, src = plan.beyond(x_hi, WIDE, rows), plan.at_partner(x_hi, WIDE, rows)
            first = plan.beyond(hi, plan.v_cols, cols)
            for c in range(plan.v_cols):
                steps.put_potential((first + c) * long + row, edge[n][at + c, pl.ds(src, WIDE), :], WIDE)
            at += plan.v_cols
            for d in range(1, WIDE - 1):
                size = corner_depth(d)
                there = jnp.where(hi, plan.soon_at[d - 1], plan.corner - plan.soon_at[d])
                col = jnp.where(hi, WIDE + cols + d - 1, WIDE - d)
                h0[pl.ds(col * long + plan.beyond(x_hi, size, rows), size)] = edge[n][pl.ds(at + there, size)]

    def clear(h):
        steps.clear_cols(h)
        if nx > 1:
            steps.clear_rows(h)

    clear(h0)
    for m in (1, 2, 3):
        steps.step(1, steps.both_sides(False, m), 4, steps.full(6 - 2 * m), 4)
    steps.step(1, steps.both_sides(True, 1), 4, steps.outside(6), 4)
    clear(levels[1])
    for m in (1, 2):
        steps.step(2, steps.both_sides(False, m), 4, steps.full(4 - 2 * m), 4)
    steps.step(2, steps.both_sides(True, 1), 4, steps.full(4), 4)
    steps.step(2, steps.both_sides(True, 2), 4, steps.outside(4), 4)
    clear(levels[2])
    steps.step(3, steps.both_sides(False, 1), 4, steps.full(0), 4)
    for m in (1, 2):
        steps.step(3, steps.both_sides(True, m), 4, steps.full(2), 4)
    steps.step(3, WIDE + 4, cols - 8, steps.outside(2), 4)
    clear(levels[3])

    sign = jnp.where(lax.broadcasted_iota(jnp.int32, (f, LANES), 0) < plan.bands, 1.0, -1.0)

    def total(s, g):
        a = [(s / 24.0) ** k for k in range(ORDER + 1)]
        even = g[0] - (a[2] / 2) * g[2] + (a[4] / 24) * g[4]
        odd = (a[3] / 6 * sign) * g[3] - (a[1] * sign) * g[1]
        return even + pltpu.roll(odd, plan.bands, 0)

    @pl.loop(0, cols, unroll=divisor(cols, 12))
    def _(c):
        def finish(at, t, value):
            g = [h[at] for h in levels] + [value]
            half = total(step_length / 2, g)
            cell = c * rows + t
            if final:
                flat[pl.ds(pl.multiple_of(cell * f, f), f), :] = half
            else:
                half_ref[cell] = half
                full = total(step_length, g)
                flat[pl.ds(pl.multiple_of(cell * f, f), f), :] = full * full

        steps.image(levels[-1], (WIDE + c) * long + WIDE, rows, finish)

    if final:
        v_out[...] = v_here[...]
        for c in range(cols):
            for p in range(plan.parts):
                for b in range(plan.bands):
                    first = c * rows * f + p * plan.bands + b
                    orb_ref[p, b, c] = flat[pl.ds(first, rows, stride=f), :]
    else:
        for c in range(cols):
            parts = [flat[pl.ds(c * rows * f + n, rows, stride=f), :] for n in range(f)]
            while len(parts) > 1:
                parts = [sum(parts[n : n + 2]) for n in range(0, len(parts), 2)]
            dens_ref[c] = parts[0]
        pack(plan, half_ref, packed)


def call(kernel, outs, scratch=(), limit=8, alias=0):
    spec = pl.BlockSpec(memory_space=pltpu.VMEM)
    return lambda *args: pl.pallas_call(
        kernel,
        out_shape=[jax.ShapeDtypeStruct(s, jnp.float32) for s in outs],
        in_specs=[spec] * len(args),
        out_specs=[spec] * len(outs),
        scratch_shapes=list(scratch),
        input_output_aliases={n: n for n in range(alias)},
        compiler_params=pltpu.CompilerParams(vmem_limit_bytes=limit << 20),
    )(*args)


def solution(mesh):
    def body(orbitals, external):
        orbitals, external = jnp.swapaxes(orbitals, 2, 3), jnp.swapaxes(external, 0, 1)
        plan = Plan(mesh, orbitals.shape)
        f, cells = plan.fields, plan.cells
        field_shape, plane = (cells, f, LANES), (plan.cols, plan.rows, LANES)
        wide = (plan.wide_cells, f, LANES)
        nx, ny = len(plan.xs), len(plan.ys)
        soon, late = plan.soon_at[-1], plan.late_at[-1]
        packed = [wide] * ny + [(soon, f, LANES)] * nx + [(late, f, LANES)] * nx

        fields, dens, *out = call(
            functools.partial(enter_kernel, plan),
            [field_shape, plane] + packed,
            [pltpu.VMEM((cells * f, LANES), jnp.float32)],
        )(orbitals)

        extended = (plan.ext_rows * plan.ext_cols, f, LANES)

        def load(ext_ref, out_ref):
            out_ref[...] = ext_ref[...]

        (external,) = call(load, [plane])(external)

        def gather(fields, dens, out):
            def swap(value, **kinds):
                return plan.swap(value, **kinds)

            big = [swap(v, ky=k) for k, v in zip(plan.ys, out)]
            soon = [swap(v, kx=k) for k, v in zip(plan.xs, out[ny:])]
            late = [swap(v, kx=k) for k, v in zip(plan.xs, out[ny + nx :])]
            dens = dens + swap(dens, flip=1)
            more = [swap(dens, flip=b) for b in range(2, plan.groups, 2)]
            (v_here,) = call(potential_kernel, [plane])(external, dens, *more)
            v_there = [swap(v_here, kx=k, flip=1) for k in plan.xs]
            edge = call(
                functools.partial(edge_kernel, plan), [(plan.edge_cells, f, LANES)] * ny
            )(v_here, *v_there, *soon)
            edge = [swap(v, ky=k) for k, v in zip(plan.ys, edge)]
            inside = call(
                functools.partial(inner_kernel, plan), [extended] * (ORDER + 1), limit=4
            )(fields, *soon, *late, *big, v_here, *v_there)
            return [*inside, *edge], v_here

        blocks = [extended] * (ORDER + 1)
        arrived, _ = gather(fields, dens, out)
        half, dens, *out = call(
            functools.partial(evolve_kernel, plan, False),
            blocks + [field_shape, plane] + packed,
            [pltpu.VMEM((cells * f, LANES), jnp.float32)],
            limit=4,
            alias=len(blocks),
        )(*arrived)[len(blocks) :]
        arrived, v_here = gather(half, dens, out)
        result, potential = call(
            functools.partial(evolve_kernel, plan, True),
            blocks + [orbitals.shape, plane],
            [pltpu.VMEM((cells * f, LANES), jnp.float32)],
            limit=4,
            alias=len(blocks),
        )(*arrived, v_here)[len(blocks) :]
        return jnp.swapaxes(result, 2, 3), jnp.swapaxes(potential, 0, 1)

    in_specs = (P(None, "band", "gx", "gy", None), P("gx", "gy", None))
    out_specs = (P(None, "band", "gx", "gy", None), P("gx", "gy", None))
    return jax.shard_map(body, mesh=mesh, in_specs=in_specs, out_specs=out_specs, check_vma=False)
```
